32 devices in a mesh: data: 1 (over z), seq: 32 (over y, x, core).
Axes of the slice: x: 4, y: 4, z: 1, core: 2. Of those that a mesh axis runs over, the one named last changes fastest.
The devices are a block of a 4x4x8 slice.
Arguments:
- x: bfloat16 [2048, 2560], P(('data', 'seq'))
- g1: float32 [2560], replicated
- b1: float32 [2560], replicated
- g2: float32 [2560], replicated
- b2: float32 [2560], replicated
- wqkv: bfloat16 [2560, 7680], replicated
- wo: bfloat16 [32, 80, 2560], replicated
- w1: bfloat16 [2560, 10240], replicated
- w2: bfloat16 [10240, 2560], replicated
Outputs:
- output: bfloat16 [2048, 2560], P(('data', 'seq'))
All inputs are finite; a program needn't handle non-finite values.
Results may differ from the reference program's by a relative error of at most 0.00237603.
Values are sent between devices in bfloat16 or wider.
A program may use at most 768 MiB of HBM per device.

```python
import jax
import jax.numpy as jnp
from jax import lax

S = 2048
D = 2560
H = 32
DH = 80
F = 10240
QB = 128

EPS = 1e-5
SCALE = DH ** -0.5
NEG = -1e30


def setup_inputs(seed: int = 0, part: int = 0) -> dict:
    key = jax.random.PRNGKey(seed)
    k_shared, k_part = jax.random.split(key)
    kp = jax.random.fold_in(k_part, part)
    kx, ku, kf, kph = jax.random.split(kp, 4)
    ks = jax.random.split(k_shared, 8)
    nf = 4
    t = jnp.arange(S, dtype=jnp.float32) / S
    freq = jax.random.uniform(kf, (nf,), jnp.float32, 0.25, 2.0)
    phase = jax.random.uniform(kph, (nf,), jnp.float32, 0.0, 6.2831853)
    waves = jnp.sin(6.2831853 * freq[None, :] * t[:, None] + phase[None, :])
    u = jax.random.normal(ku, (nf, D), jnp.float32)
    smooth = jnp.dot(waves, u) * (2.0 / nf) ** 0.5
    x = 0.6 * jax.random.normal(kx, (S, D), jnp.float32) + smooth

    def w(k, shape, fan_in):
        return (jax.random.normal(k, shape, jnp.float32) * fan_in ** -0.5).astype(jnp.bfloat16)

    return {
        "x": x.astype(jnp.bfloat16),
        "g1": 1.0 + 0.2 * jax.random.normal(ks[0], (D,), jnp.float32),
        "b1": 0.2 * jax.random.normal(ks[1], (D,), jnp.float32),
        "g2": 1.0 + 0.2 * jax.random.normal(ks[2], (D,), jnp.float32),
        "b2": 0.2 * jax.random.normal(ks[3], (D,), jnp.float32),
        "wqkv": w(ks[4], (D, 3 * H * DH), D),
        "wo": w(ks[5], (H, DH, D), H * DH),
        "w1": w(ks[6], (D, F), D),
        "w2": w(ks[7], (F, D), F),
    }


def _layer_norm(x, g, b):
    xf = x.astype(jnp.float32)
    mu = jnp.mean(xf, axis=-1, keepdims=True)
    var = jnp.mean(jnp.square(xf - mu), axis=-1, keepdims=True)
    return ((xf - mu) * lax.rsqrt(var + EPS) * g + b).astype(jnp.bfloat16)


def _rope(t, pos):
    half = DH // 2
    inv = 10000.0 ** (-2.0 * jnp.arange(half, dtype=jnp.float32) / DH)
    ang = pos.astype(jnp.float32)[:, None] * inv[None, :]
    cos = jnp.cos(ang)[:, None, :]
    sin = jnp.sin(ang)[:, None, :]
    tf = t.astype(jnp.float32)
    a, b = tf[..., :half], tf[..., half:]
    return jnp.concatenate([a * cos - b * sin, b * cos + a * sin], axis=-1).astype(jnp.bfloat16)


def _head_attention(qh, kh, vh):
    rows = jnp.arange(S).reshape(S // QB, QB)
    cols = jnp.arange(S)

    def block(args):
        qb, rb = args
        s = jnp.dot(qb, kh.T, preferred_element_type=jnp.float32) * SCALE
        s = jnp.where(cols[None, :] <= rb[:, None], s, NEG)
        p = jax.nn.softmax(s, axis=-1).astype(jnp.bfloat16)
        return jnp.dot(p, vh, preferred_element_type=jnp.float32).astype(jnp.bfloat16)

    return lax.map(block, (qh.reshape(S // QB, QB, DH), rows)).reshape(S, DH)


def reference(x, g1, b1, g2, b2, wqkv, wo, w1, w2):
    pos = jnp.arange(S)
    a = _layer_norm(x, g1, b1)
    qkv = jnp.dot(a, wqkv, preferred_element_type=jnp.float32).astype(jnp.bfloat16).reshape(S, 3, H, DH)
    q = _rope(qkv[:, 0], pos)
    k = _rope(qkv[:, 1], pos)
    v = qkv[:, 2]
    o = lax.map(lambda t: _head_attention(t[0], t[1], t[2]),
                (q.transpose(1, 0, 2), k.transpose(1, 0, 2), v.transpose(1, 0, 2)))
    o = o.transpose(1, 0, 2).reshape(S, H * DH)
    attn = jnp.dot(o, wo.reshape(H * DH, D), preferred_element_type=jnp.float32)
    m = _layer_norm(x, g2, b2)
    h = jax.nn.gelu(jnp.dot(m, w1, preferred_element_type=jnp.float32), approximate=False).astype(jnp.bfloat16)
    mlp = jnp.dot(h, w2, preferred_element_type=jnp.float32)
    return (x.astype(jnp.float32) + attn + mlp).astype(jnp.bfloat16)
```

```python
import functools
import math

import jax
import jax.numpy as jnp
import numpy as np
from jax import lax
from jax.experimental import pallas as pl
from jax.experimental.pallas import tpu as pltpu
from jax.sharding import PartitionSpec as P

EPS = 1e-5
NEG = -1e30
F32 = jnp.float32
BF16 = jnp.bfloat16
MESH = pl.DeviceIdType.MESH
SLOTS = 6
GH = 8
KB = 512


def _gelu(x):
    return 0.5 * x * (1.0 + lax.erf(x * np.float32(math.sqrt(0.5))))


def _kernel(dims, x_hbm, g1_hbm, b1_hbm, g2_hbm, b2_hbm, inv_hbm, wqkv, wo, w1, w2, y_hbm,
            xall, gb, inv_v, a_v, m_v, h_v, aw, bw, sbuf, rbuf, obuf, orecv, ocat, yacc, yrecv, ybuf, cs,
            small_sem, a_sem, b_sem, xs_sem, xr_sem, qs_sem, qr_sem, os_sem, or_sem, ys_sem, yr_sem, loc_sem, out_sem):
    r, d, nh, dh, f, nchip = dims
    half = dh // 2
    dc = d // 2
    fc = f // 2
    cw = GH * dh
    ngrp = nchip // GH
    nm = fc // cw
    r2 = 2 * r
    s = lax.axis_index("seq")
    c = lax.rem(s, 2)
    me = lax.div(s, 2)
    partner = s + 1 - 2 * c

    def dev(chip):
        return {"seq": 2 * chip + c}

    barrier = pltpu.get_barrier_semaphore()
    pl.semaphore_signal(barrier, inc=1, device_id={"seq": partner}, device_id_type=MESH)
    for i in range(1, nchip):
        pl.semaphore_signal(barrier, inc=1, device_id=dev(lax.rem(me + i, nchip)), device_id_type=MESH)

    def qkv_copy(g, t):
        col = pl.multiple_of(t * d + c * dc + g * cw, 128)
        n = 3 * g + t
        return pltpu.make_async_copy(wqkv.at[:, pl.ds(col, cw)], aw.at[n], a_sem.at[n])

    def w1_copy(m):
        col = pl.multiple_of(c * fc + m * cw, 128)
        n = lax.rem(m, SLOTS)
        return pltpu.make_async_copy(w1.at[:, pl.ds(col, cw)], aw.at[n], a_sem.at[n])

    nb2 = nm
    nbo = dc // cw

    def b_copy(n):
        if n < nb2:
            return pltpu.make_async_copy(w2.at[pl.ds(pl.multiple_of(c * fc + n * cw, 128), cw), :],
                                         bw.at[pl.ds(n * cw, cw), :], b_sem.at[n])
        k = n - nb2
        return pltpu.make_async_copy(wo.at[pl.ds(pl.multiple_of(c * dc + k * cw, 128), cw), :],
                                     bw.at[pl.ds(n * cw, cw), :], b_sem.at[n])

    mine = pl.ds(pl.multiple_of(c * r, r), r)
    smalls = [
        pltpu.make_async_copy(x_hbm, xall.at[mine, :], small_sem.at[0]),
        pltpu.make_async_copy(g1_hbm, gb.at[0], small_sem.at[1]),
        pltpu.make_async_copy(b1_hbm, gb.at[1], small_sem.at[2]),
        pltpu.make_async_copy(g2_hbm, gb.at[2], small_sem.at[3]),
        pltpu.make_async_copy(b2_hbm, gb.at[3], small_sem.at[4]),
        pltpu.make_async_copy(inv_hbm, inv_v, small_sem.at[5]),
    ]
    for cp in smalls:
        cp.start()
    for g in range(ngrp):
        for t in range(3):
            qkv_copy(g, t).start()
    for n in range(2):
        b_copy(n).start()

    smalls[5].wait()
    pos = (me * r2 + lax.broadcasted_iota(jnp.int32, (r2, 128), 0)).astype(F32)
    ang = pos * inv_v[0:1, :]
    cos = jnp.cos(ang)
    sin = jnp.sin(ang)
    lane = lax.broadcasted_iota(jnp.int32, (r2, 128), 1)
    sin = jnp.where(lane < half, -sin, sin)
    cs[0] = jnp.concatenate([cos[:, :dh]] * GH, axis=1)
    cs[1] = jnp.concatenate([sin[:, :dh]] * GH, axis=1)

    for cp in smalls[:5]:
        cp.wait()
    pl.semaphore_wait(barrier, nchip)
    xcopy = pltpu.make_async_remote_copy(
        src_ref=xall.at[mine, :], dst_ref=xall.at[mine, :], send_sem=xs_sem, recv_sem=xr_sem,
        device_id={"seq": partner}, device_id_type=MESH)
    xcopy.start()
    xcopy.wait()

    xf = xall[...].astype(F32)
    mu = jnp.mean(xf, axis=-1, keepdims=True)
    xc = xf - mu
    var = jnp.mean(jnp.square(xc), axis=-1, keepdims=True)
    xn = xc * lax.rsqrt(var + EPS)
    a_v[...] = (xn * gb[0] + gb[1]).astype(BF16)
    m_v[...] = (xn * gb[2] + gb[3]).astype(BF16)

    lane_c = lax.rem(lax.broadcasted_iota(jnp.int32, (r2, cw), 1), dh)

    def rope(t):
        tf = t.astype(F32)
        up = pltpu.roll(tf, cw - half, axis=1)
        dn = pltpu.roll(tf, half, axis=1)
        rot = jnp.where(lane_c < half, up, dn)
        return (tf * cs[0] + rot * cs[1]).astype(BF16)

    def q_send(src, chip):
        return pltpu.make_async_remote_copy(
            src_ref=sbuf.at[chip], dst_ref=rbuf.at[pl.ds(pl.multiple_of(src * r2, r2), r2), :],
            send_sem=qs_sem.at[chip], recv_sem=qr_sem.at[src], device_id=dev(chip), device_id_type=MESH)

    def q_local():
        return pltpu.make_async_copy(
            sbuf.at[me], rbuf.at[pl.ds(pl.multiple_of(me * r2, r2), r2), :], loc_sem.at[0])

    for g in range(ngrp):
        parts = []
        for t in range(3):
            qkv_copy(g, t).wait()
            val = jnp.dot(a_v[...], aw[3 * g + t], preferred_element_type=F32).astype(BF16)
            w1_copy(3 * g + t).start()
            parts.append(rope(val) if t < 2 else val)
        for j in range(GH):
            sl = slice(j * dh, (j + 1) * dh)
            sbuf[g * GH + j] = jnp.concatenate(
                [parts[0][:, sl], parts[1][:, sl], parts[2][:, sl], jnp.zeros((r2, 256 - 3 * dh), BF16)], axis=1)

        def send(j, carry):
            chip = g * GH + lax.rem(j + me, GH)

            @pl.when(chip != me)
            def _():
                q_send(me, chip).start()

            @pl.when(chip == me)
            def _():
                q_local().start()
            return carry

        lax.fori_loop(0, GH, send, 0)

    def mlp1(m, carry):
        w1_copy(m).wait()
        t = jnp.dot(m_v[...], aw[lax.rem(m, SLOTS)], preferred_element_type=F32)
        h_v[:, pl.ds(pl.multiple_of(m * cw, 128), cw)] = _gelu(t).astype(BF16)

        @pl.when(m < nm - SLOTS)
        def _():
            w1_copy(m + SLOTS).start()
        return carry

    lax.fori_loop(0, nm - SLOTS, mlp1, 0)
    for n in range(2, nb2 + nbo):
        b_copy(n).start()
    lax.fori_loop(nm - SLOTS, nm, mlp1, 0)

    q_local().wait()

    def q_wait(i, carry):
        chip = lax.rem(me + i, nchip)
        q_send(chip, chip).wait()
        return carry

    lax.fori_loop(1, nchip, q_wait, 0)

    scale = dh ** -0.5
    qper = KB // r2

    def o_send(src, chip):
        return pltpu.make_async_remote_copy(
            src_ref=obuf.at[chip], dst_ref=orecv.at[src],
            send_sem=os_sem.at[chip], recv_sem=or_sem.at[src], device_id=dev(chip), device_id_type=MESH)

    def o_local():
        return pltpu.make_async_copy(obuf.at[me], orecv.at[me], loc_sem.at[1])

    def attend(i, carry):
        j = lax.rem(me + 1 + i, nchip)
        row0 = pl.multiple_of(j * r2, r2)

        def case(nk):
            kn = nk * KB
            q = rbuf[pl.ds(row0, r2), 0:128]
            lq = jnp.concatenate([jnp.zeros((r2, dh), BF16), q[:, :dh], jnp.zeros((r2, 256 - 2 * dh), BF16)], axis=1)
            sc = lax.dot_general(lq, rbuf[0:kn, :], (((1,), (1,)), ((), ())), preferred_element_type=F32) * scale
            last = sc[:, kn - KB:]
            rows = row0 + lax.broadcasted_iota(jnp.int32, (r2, KB), 0)
            cols = (kn - KB) + lax.broadcasted_iota(jnp.int32, (r2, KB), 1)
            last = jnp.where(cols <= rows, last, NEG)
            sc = last if nk == 1 else jnp.concatenate([sc[:, :kn - KB], last], axis=1)
            mx = jnp.max(sc, axis=-1, keepdims=True)
            e = jnp.exp(sc - mx)
            p = (e * (1.0 / jnp.sum(e, axis=-1, keepdims=True))).astype(BF16)
            o = jnp.dot(p, rbuf[0:kn, 128:256], preferred_element_type=F32)
            obuf[j] = pltpu.roll(o, 128 - (2 * dh - 128), axis=1).astype(BF16)

        for nk in range(1, nchip // qper + 1):
            pl.when(lax.div(j, qper) == nk - 1)(functools.partial(case, nk))

        @pl.when(j != me)
        def _():
            o_send(me, j).start()

        @pl.when(j == me)
        def _():
            o_local().start()
        return carry

    lax.fori_loop(0, nchip, attend, 0)

    for n in range(nb2):
        b_copy(n).wait()
    nt = 256

    def mlp2(n, carry):
        cols = pl.ds(pl.multiple_of(n * nt, 128), nt)
        t = jnp.dot(h_v[...], bw[0:fc, cols], preferred_element_type=F32)
        yacc[:, :, cols] = t.reshape(2, r, nt)
        return carry

    lax.fori_loop(0, d // nt, mlp2, 0)

    o_local().wait()

    def o_wait(i, carry):
        chip = lax.rem(me + i, nchip)
        o_send(chip, chip).wait()
        return carry

    lax.fori_loop(1, nchip, o_wait, 0)
    ocat[...] = jnp.concatenate([orecv[j][:, :dh] for j in range(nchip)], axis=1)
    for n in range(nb2, nb2 + nbo):
        b_copy(n).wait()

    ny = d // cw

    def y_send(n):
        cols = pl.ds(pl.multiple_of(n * cw, 128), cw)
        return pltpu.make_async_remote_copy(
            src_ref=yacc.at[1 - c, :, cols], dst_ref=yrecv.at[:, cols],
            send_sem=ys_sem.at[n], recv_sem=yr_sem.at[n], device_id={"seq": partner}, device_id_type=MESH)

    def proj(n, carry):
        cols = pl.ds(pl.multiple_of(n * cw, 128), cw)
        t = jnp.dot(ocat[...], bw[fc:fc + dc, cols], preferred_element_type=F32)
        yacc[:, :, cols] = yacc[:, :, cols] + t.reshape(2, r, cw)
        y_send(n).start()
        return carry

    lax.fori_loop(0, ny, proj, 0)

    def finish(n, carry):
        cols = pl.ds(pl.multiple_of(n * cw, 128), cw)
        y_send(n).wait()
        ybuf[:, cols] = (xall[mine, cols].astype(F32) + yacc[c, :, cols] + yrecv[:, cols]).astype(BF16)
        return carry

    lax.fori_loop(0, ny, finish, 0)
    out = pltpu.make_async_copy(ybuf, y_hbm, out_sem)
    out.start()
    out.wait()


def solution(mesh):
    nseq = mesh.shape["seq"]
    nchip = nseq // 2

    def local(x, g1, b1, g2, b2, wqkv, wo, w1, w2):
        r, d = x.shape
        nh, dh, _ = wo.shape
        f = w1.shape[1]
        if nh != nseq or nchip % GH or (KB % (2 * r)):
            raise ValueError("unsupported sizes")
        half = dh // 2
        inv = 10000.0 ** (-2.0 * np.arange(half) / dh)
        inv = np.concatenate([inv, inv, np.zeros(128 - dh)]).astype(np.float32)
        inv = jnp.asarray(np.tile(inv[None], (8, 1)))
        r2, cw, dc, fc = 2 * r, GH * dh, d // 2, f // 2
        nb = (fc + dc) // cw
        dma = pltpu.SemaphoreType.DMA
        flops = 2 * r2 * (d * 3 * dc + d * fc * 2 + dc * d)
        return pl.pallas_call(
            functools.partial(_kernel, (r, d, nh, dh, f, nchip)),
            out_shape=jax.ShapeDtypeStruct((r, d), BF16),
            in_specs=[pl.BlockSpec(memory_space=pl.ANY)] * 10,
            out_specs=pl.BlockSpec(memory_space=pl.ANY),
            scratch_shapes=[
                pltpu.VMEM((r2, d), BF16),
                pltpu.VMEM((4, 1, d), F32),
                pltpu.VMEM((8, 128), F32),
                pltpu.VMEM((r2, d), BF16),
                pltpu.VMEM((r2, d), BF16),
                pltpu.VMEM((r2, fc), BF16),
                pltpu.VMEM((SLOTS, d, cw), BF16),
                pltpu.VMEM((fc + dc, d), BF16),
                pltpu.VMEM((nchip, r2, 256), BF16),
                pltpu.VMEM((nchip * r2, 256), BF16),
                pltpu.VMEM((nchip, r2, 128), BF16),
                pltpu.VMEM((nchip, r2, 128), BF16),
                pltpu.VMEM((r2, dc), BF16),
                pltpu.VMEM((2, r, d), F32),
                pltpu.VMEM((r, d), F32),
                pltpu.VMEM((r, d), BF16),
                pltpu.VMEM((2, r2, cw), F32),
                dma((6,)), dma((SLOTS,)), dma((nb,)), dma, dma,
                dma((nchip,)), dma((nchip,)), dma((nchip,)), dma((nchip,)),
                dma((d // cw,)), dma((d // cw,)), dma((2,)), dma,
            ],
            compiler_params=pltpu.CompilerParams(
                collective_id=0, has_side_effects=True, vmem_limit_bytes=67043328),
            cost_estimate=pl.CostEstimate(flops=flops, bytes_accessed=2 * (d * 3 * dc + d * f + dc * d), transcendentals=0),
            name="layer",
        )(x, g1.reshape(1, d), b1.reshape(1, d), g2.reshape(1, d), b2.reshape(1, d), inv,
          wqkv, wo.reshape(nh * dh, d), w1, w2)

    rows = P(("data", "seq"), None)
    rep = P()
    return jax.shard_map(local, mesh=mesh,
                         in_specs=(rows, rep, rep, rep, rep, rep, rep, rep, rep),
                         out_specs=rows, check_vma=False)
```

```python
import functools
import math

import jax
import jax.numpy as jnp
import numpy as np
from jax import lax
from jax.experimental import pallas as pl
from jax.experimental.pallas import tpu as pltpu
from jax.sharding import PartitionSpec as P

EPS = 1e-5
NEG = -1e30
F32 = jnp.float32
BF16 = jnp.bfloat16
MESH = pl.DeviceIdType.MESH
SLOTS = 6
GH = 8
KB = 512


def _gelu(x):
    return 0.5 * x * (1.0 + lax.erf(x * np.float32(math.sqrt(0.5))))


def _kernel(dims, x_hbm, g1_hbm, b1_hbm, g2_hbm, b2_hbm, inv_hbm, wqkv, wo, w1, w2, y_hbm,
            xall, g1_v, b1_v, g2_v, b2_v, inv_v, a_v, m_v, t_v, h_v, aw, bw, sbuf, rbuf, obuf, orecv, ocat, yacc, yrecv, ybuf, cs,
            small_sem, a_sem, b_sem, xs_sem, xr_sem, qs_sem, qr_sem, os_sem, or_sem, ys_sem, yr_sem, loc_sem, out_sem):
    r, d, nh, dh, f, nchip = dims
    half = dh // 2
    dc = d // 2
    fc = f // 2
    cw = GH * dh
    ngrp = nchip // GH
    nm = fc // cw
    r2 = 2 * r
    s = lax.axis_index("seq")
    c = lax.rem(s, 2)
    me = lax.div(s, 2)
    partner = s + 1 - 2 * c

    def dev(chip):
        return {"seq": 2 * chip + c}

    def group(g):
        return lax.rem(g + lax.div(2 * me, nchip) + 1, ngrp)

    def qkv_copy(g, t):
        col = pl.multiple_of(t * d + c * dc + group(g) * cw, 128)
        n = 3 * g + t
        return pltpu.make_async_copy(wqkv.at[:, pl.ds(col, cw)], aw.at[n], a_sem.at[n])

    def w1_copy(m):
        col = pl.multiple_of(c * fc + m * cw, 128)
        n = lax.rem(m, SLOTS)
        return pltpu.make_async_copy(w1.at[:, pl.ds(col, cw)], aw.at[n], a_sem.at[n])

    nb2 = nm
    nbo = dc // cw

    def b_copy(n):
        if n < nb2:
            return pltpu.make_async_copy(w2.at[pl.ds(pl.multiple_of(c * fc + n * cw, 128), cw), :],
                                         bw.at[pl.ds(n * cw, cw), :], b_sem.at[n])
        k = n - nb2
        return pltpu.make_async_copy(wo.at[pl.ds(pl.multiple_of(c * dc + k * cw, 128), cw), :],
                                     bw.at[pl.ds(n * cw, cw), :], b_sem.at[n])

    smalls = [
        pltpu.make_async_copy(x_hbm, xall.at[c], small_sem.at[0]),
        pltpu.make_async_copy(g1_hbm, g1_v, small_sem.at[1]),
        pltpu.make_async_copy(b1_hbm, b1_v, small_sem.at[2]),
        pltpu.make_async_copy(g2_hbm, g2_v, small_sem.at[3]),
        pltpu.make_async_copy(b2_hbm, b2_v, small_sem.at[4]),
        pltpu.make_async_copy(inv_hbm, inv_v, small_sem.at[5]),
    ]
    for cp in smalls:
        cp.start()
    for g in range(ngrp):
        for t in range(3):
            qkv_copy(g, t).start()
    for n in range(2):
        b_copy(n).start()

    barrier = pltpu.get_barrier_semaphore()
    pl.semaphore_signal(barrier, inc=1, device_id={"seq": partner}, device_id_type=MESH)
    for i in range(1, nchip):
        pl.semaphore_signal(barrier, inc=1, device_id=dev(lax.rem(me + i, nchip)), device_id_type=MESH)

    for cp in smalls:
        cp.wait()
    pos = (me * r2 + lax.broadcasted_iota(jnp.int32, (r2, 128), 0)).astype(F32)
    ang = pos * inv_v[0:1, :]
    cos = jnp.cos(ang)
    sin = jnp.sin(ang)
    lane = lax.broadcasted_iota(jnp.int32, (r2, 128), 1)
    sin = jnp.where(lane < half, -sin, sin)
    cs[0] = jnp.concatenate([cos[:, :dh]] * GH, axis=1)
    cs[1] = jnp.concatenate([sin[:, :dh]] * GH, axis=1)

    def norms(which):
        xf = xall[which].astype(F32)
        mu = jnp.mean(xf, axis=-1, keepdims=True)
        xc = xf - mu
        var = jnp.mean(jnp.square(xc), axis=-1, keepdims=True)
        xn = xc * lax.rsqrt(var + EPS)
        a_v[which] = (xn * g1_v[...].reshape(1, d) + b1_v[...].reshape(1, d)).astype(BF16)
        m_v[which] = (xn * g2_v[...].reshape(1, d) + b2_v[...].reshape(1, d)).astype(BF16)

    norms(c)

    pl.semaphore_wait(barrier, nchip)
    xcopy = pltpu.make_async_remote_copy(
        src_ref=xall.at[c], dst_ref=xall.at[c], send_sem=xs_sem, recv_sem=xr_sem,
        device_id={"seq": partner}, device_id_type=MESH)
    xcopy.start()
    xcopy.wait()
    norms(1 - c)

    lane_c = lax.rem(lax.broadcasted_iota(jnp.int32, (r2, cw), 1), dh)

    def rope(t):
        tf = t.astype(F32)
        up = pltpu.roll(tf, cw - half, axis=1)
        dn = pltpu.roll(tf, half, axis=1)
        rot = jnp.where(lane_c < half, up, dn)
        return (tf * cs[0] + rot * cs[1]).astype(BF16)

    def q_send(src, chip):
        return pltpu.make_async_remote_copy(
            src_ref=sbuf.at[chip], dst_ref=rbuf.at[pl.ds(pl.multiple_of(src * r2, r2), r2), :],
            send_sem=qs_sem.at[chip], recv_sem=qr_sem.at[src], device_id=dev(chip), device_id_type=MESH)

    def q_local():
        return pltpu.make_async_copy(
            sbuf.at[me], rbuf.at[pl.ds(pl.multiple_of(me * r2, r2), r2), :], loc_sem.at[0])

    for g in range(ngrp):
        gg = group(g)
        for t in range(3):
            qkv_copy(g, t).wait()
        a = a_v[...].reshape(r2, d)
        parts = [jnp.dot(a, aw[3 * g + t], preferred_element_type=F32).astype(BF16) for t in range(3)]
        parts = [rope(parts[0]), rope(parts[1]), parts[2]]
        for j in range(GH):
            sl = slice(j * dh, (j + 1) * dh)
            sbuf[gg * GH + j] = jnp.concatenate(
                [parts[0][:, sl], parts[1][:, sl], parts[2][:, sl], jnp.zeros((r2, 256 - 3 * dh), BF16)], axis=1)
        for t in range(3):
            w1_copy(3 * g + t).start()

        def send(j, carry):
            chip = gg * GH + lax.rem(j + me, GH)

            @pl.when(chip != me)
            def _():
                q_send(me, chip).start()

            @pl.when(chip == me)
            def _():
                q_local().start()
            return carry

        lax.fori_loop(0, GH, send, 0)

    def up(m):
        t_v[lax.rem(m, 2)] = jnp.dot(m_v[...].reshape(r2, d), aw[lax.rem(m, SLOTS)], preferred_element_type=F32)

    def act(m):
        h_v[:, pl.ds(pl.multiple_of(m * cw, 128), cw)] = _gelu(t_v[lax.rem(m, 2)]).astype(BF16)

    w1_copy(0).wait()
    up(0)
    w1_copy(SLOTS).start()

    def mlp1(m, carry):
        w1_copy(m).wait()
        up(m)
        act(m - 1)

        @pl.when(m < nm - SLOTS)
        def _():
            w1_copy(m + SLOTS).start()
        return carry

    lax.fori_loop(1, nm - SLOTS, mlp1, 0)
    for n in range(2, nb2 + nbo):
        b_copy(n).start()
    lax.fori_loop(nm - SLOTS, nm, mlp1, 0)
    act(nm - 1)

    nt = 256
    early = nb2 // 2

    def down(k0, k1, first):
        def body(n, carry):
            cols = pl.ds(pl.multiple_of(n * nt, 128), nt)
            t = jnp.dot(h_v[:, k0:k1], bw[k0:k1, cols], preferred_element_type=F32).reshape(2, r, nt)
            yacc[:, :, cols] = t if first else yacc[:, :, cols] + t
            return carry

        lax.fori_loop(0, d // nt, body, 0)

    for n in range(early):
        b_copy(n).wait()
    down(0, early * cw, True)

    q_local().wait()

    def q_wait(i, carry):
        chip = lax.rem(me + i, nchip)
        q_send(chip, chip).wait()
        return carry

    lax.fori_loop(1, nchip, q_wait, 0)

    scale = dh ** -0.5
    qper = KB // r2

    def o_send(src, chip):
        return pltpu.make_async_remote_copy(
            src_ref=obuf.at[chip], dst_ref=orecv.at[src],
            send_sem=os_sem.at[chip], recv_sem=or_sem.at[src], device_id=dev(chip), device_id_type=MESH)

    def o_local():
        return pltpu.make_async_copy(obuf.at[me], orecv.at[me], loc_sem.at[1])

    nq = nchip // qper
    og = r2 // 16

    def attend(i, carry):
        u = lax.rem(me + i, qper)
        blocks = [qper * n + u for n in range(nq)]
        row0 = [pl.multiple_of(j * r2, r2) for j in blocks]
        lq = []
        for n in range(nq):
            q = rbuf[pl.ds(row0[n], r2), 0:128]
            lq.append(jnp.concatenate(
                [jnp.zeros((r2, dh), BF16), q[:, :dh], jnp.zeros((r2, 256 - 2 * dh), BF16)], axis=1))
        rows = u * r2 + lax.broadcasted_iota(jnp.int32, (r2, KB), 0)
        cols = lax.broadcasted_iota(jnp.int32, (r2, KB), 1)
        seen = cols <= rows
        sc = [[] for _ in range(nq)]
        for k in range(nq):
            t = lax.dot_general(jnp.concatenate(lq[k:], axis=0), rbuf[k * KB:(k + 1) * KB, :],
                                (((1,), (1,)), ((), ())), preferred_element_type=F32)
            for n in range(k, nq):
                tn = t[(n - k) * r2:(n - k + 1) * r2]
                sc[n].append(jnp.where(seen, tn, NEG) if n == k else tn)
        for n in range(nq):
            mx = functools.reduce(jnp.maximum, sc[n])
            mx = jnp.max(mx, axis=-1, keepdims=True)
            e = [jnp.exp((t - mx) * scale) for t in sc[n]]
            inv_l = 1.0 / jnp.sum(functools.reduce(jnp.add, e), axis=-1, keepdims=True)
            p = jnp.concatenate([(t * inv_l).astype(BF16) for t in e], axis=1)
            o = jnp.dot(p, rbuf[0:(n + 1) * KB, 128:256], preferred_element_type=F32)
            v0 = 2 * dh - 128
            obuf[blocks[n]] = jnp.concatenate(
                [o[16 * g:16 * (g + 1), v0:v0 + dh] for g in range(og)], axis=1).astype(BF16)

        def send(n, carry):
            j = qper * n + u

            @pl.when(j != me)
            def _():
                o_send(me, j).start()

            @pl.when(j == me)
            def _():
                o_local().start()
            return carry

        lax.fori_loop(0, nq, send, 0)
        return carry

    lax.fori_loop(0, qper, attend, 0)

    for n in range(early, nb2):
        b_copy(n).wait()
    down(early * cw, fc, False)

    o_local().wait()

    def o_wait(i, carry):
        chip = lax.rem(me + i, nchip)
        o_send(chip, chip).wait()
        return carry

    lax.fori_loop(1, nchip, o_wait, 0)
    for g in range(og):
        ocat[16 * g:16 * (g + 1), :] = jnp.concatenate(
            [orecv[j][:, g * dh:(g + 1) * dh] for j in range(nchip)], axis=1)
    for n in range(nb2, nb2 + nbo):
        b_copy(n).wait()

    ny = d // cw

    def y_send(n):
        cols = pl.ds(pl.multiple_of(n * cw, 128), cw)
        return pltpu.make_async_remote_copy(
            src_ref=yacc.at[1 - c, :, cols], dst_ref=yrecv.at[:, cols],
            send_sem=ys_sem.at[n], recv_sem=yr_sem.at[n], device_id={"seq": partner}, device_id_type=MESH)

    def proj(n, carry):
        cols = pl.ds(pl.multiple_of(n * cw, 128), cw)
        t = jnp.dot(ocat[...], bw[fc:fc + dc, cols], preferred_element_type=F32)
        yacc[:, :, cols] = yacc[:, :, cols] + t.reshape(2, r, cw)
        y_send(n).start()
        return carry

    lax.fori_loop(0, ny, proj, 0)

    def finish(n, carry):
        cols = pl.ds(pl.multiple_of(n * cw, 128), cw)
        y_send(n).wait()
        ybuf[:, cols] = (xall[c, :, cols].astype(F32) + yacc[c, :, cols] + yrecv[:, cols]).astype(BF16)
        return carry

    lax.fori_loop(0, ny, finish, 0)
    out = pltpu.make_async_copy(ybuf, y_hbm, out_sem)
    out.start()
    out.wait()


def solution(mesh):
    nseq = mesh.shape["seq"]
    nchip = nseq // 2

    def local(x, g1, b1, g2, b2, wqkv, wo, w1, w2):
        r, d = x.shape
        nh, dh, _ = wo.shape
        f = w1.shape[1]
        if nh != nseq or nchip % GH or (KB % (2 * r)):
            raise ValueError("unsupported sizes")
        half = dh // 2
        inv = 10000.0 ** (-2.0 * np.arange(half) / dh)
        inv = np.concatenate([inv, inv, np.zeros(128 - dh)]).astype(np.float32)
        inv = jnp.asarray(np.tile(inv[None], (8, 1)))
        r2, cw, dc, fc = 2 * r, GH * dh, d // 2, f // 2
        nb = (fc + dc) // cw
        dma = pltpu.SemaphoreType.DMA
        flops = 2 * r2 * (d * 3 * dc + d * fc * 2 + dc * d)
        return pl.pallas_call(
            functools.partial(_kernel, (r, d, nh, dh, f, nchip)),
            out_shape=jax.ShapeDtypeStruct((r, d), BF16),
            in_specs=[pl.BlockSpec(memory_space=pl.ANY)] * 10,
            out_specs=pl.BlockSpec(memory_space=pl.ANY),
            scratch_shapes=[
                pltpu.VMEM((2, r, d), BF16),
                pltpu.VMEM((d,), F32),
                pltpu.VMEM((d,), F32),
                pltpu.VMEM((d,), F32),
                pltpu.VMEM((d,), F32),
                pltpu.VMEM((8, 128), F32),
                pltpu.VMEM((2, r, d), BF16),
                pltpu.VMEM((2, r, d), BF16),
                pltpu.VMEM((2, r2, cw), F32),
                pltpu.VMEM((r2, fc), BF16),
                pltpu.VMEM((SLOTS, d, cw), BF16),
                pltpu.VMEM((fc + dc, d), BF16),
                pltpu.VMEM((nchip, r2, 256), BF16),
                pltpu.VMEM((nchip * r2, 256), BF16),
                pltpu.VMEM((nchip, 16, r2 // 16 * dh), BF16),
                pltpu.VMEM((nchip, 16, r2 // 16 * dh), BF16),
                pltpu.VMEM((r2, dc), BF16),
                pltpu.VMEM((2, r, d), F32),
                pltpu.VMEM((r, d), F32),
                pltpu.VMEM((r, d), BF16),
                pltpu.VMEM((2, r2, cw), F32),
                dma((6,)), dma((SLOTS,)), dma((nb,)), dma, dma,
                dma((nchip,)), dma((nchip,)), dma((nchip,)), dma((nchip,)),
                dma((d // cw,)), dma((d // cw,)), dma((2,)), dma,
            ],
            compiler_params=pltpu.CompilerParams(
                collective_id=0, has_side_effects=True, vmem_limit_bytes=67043328),
            cost_estimate=pl.CostEstimate(flops=flops, bytes_accessed=2 * (d * 3 * dc + d * f + dc * d), transcendentals=0),
            name="layer",
        )(x, g1, b1, g2, b2, inv,
          wqkv, wo.reshape(nh * dh, d), w1, w2)

    rows = P(("data", "seq"), None)
    rep = P()
    return jax.shard_map(local, mesh=mesh,
                         in_specs=(rows, rep, rep, rep, rep, rep, rep, rep, rep),
                         out_specs=rows, check_vma=False)
```

```python
import functools
import math

import jax
import jax.numpy as jnp
import numpy as np
from jax import lax
from jax.experimental import pallas as pl
from jax.experimental.pallas import tpu as pltpu
from jax.sharding import PartitionSpec as P

EPS = 1e-5
NEG = -1e30
F32 = jnp.float32
BF16 = jnp.bfloat16
MESH = pl.DeviceIdType.MESH
SLOTS = 6
GH = 8
KB = 512


def _gelu(x):
    return 0.5 * x * (1.0 + lax.erf(x * np.float32(math.sqrt(0.5))))


def _kernel(dims, x_hbm, g1_hbm, b1_hbm, g2_hbm, b2_hbm, inv_hbm, wqkv, wo, w1, w2, y_hbm,
            xall, g1_v, b1_v, g2_v, b2_v, inv_v, a_v, m_v, t_v, h_v, aw, bw, sbuf, rbuf, obuf, orecv, ocat, yacc, yrecv, ybuf, cs,
            small_sem, a_sem, b_sem, xs_sem, xr_sem, qs_sem, qr_sem, os_sem, or_sem, ys_sem, yr_sem, loc_sem, out_sem):
    r, d, nh, dh, f, nchip = dims
    half = dh // 2
    dc = d // 2
    fc = f // 2
    cw = GH * dh
    ngrp = nchip // GH
    nm = fc // cw
    r2 = 2 * r
    s = lax.axis_index("seq")
    c = lax.rem(s, 2)
    me = lax.div(s, 2)
    partner = s + 1 - 2 * c

    def dev(chip):
        return {"seq": 2 * chip + c}

    def owner(g, j):
        return ngrp * j + (j // 2 + g) % ngrp

    def group(g):
        return (me % ngrp + me // (2 * ngrp) + g + 1) % ngrp

    def qkv_copy(g, t):
        col = pl.multiple_of(t * d + c * dc + group(g) * cw, 128)
        n = 3 * g + t
        return pltpu.make_async_copy(wqkv.at[:, pl.ds(col, cw)], aw.at[n], a_sem.at[n])

    def w1_copy(m):
        col = pl.multiple_of(c * fc + m * cw, 128)
        n = lax.rem(m, SLOTS)
        return pltpu.make_async_copy(w1.at[:, pl.ds(col, cw)], aw.at[n], a_sem.at[n])

    nb2 = nm
    nbo = dc // cw

    def b_copy(n):
        if n < nb2:
            return pltpu.make_async_copy(w2.at[pl.ds(pl.multiple_of(c * fc + n * cw, 128), cw), :],
                                         bw.at[pl.ds(n * cw, cw), :], b_sem.at[n])
        k = n - nb2
        return pltpu.make_async_copy(wo.at[pl.ds(pl.multiple_of(c * dc + k * cw, 128), cw), :],
                                     bw.at[pl.ds(n * cw, cw), :], b_sem.at[n])

    smalls = [
        pltpu.make_async_copy(x_hbm, xall.at[c], small_sem.at[0]),
        pltpu.make_async_copy(g1_hbm, g1_v, small_sem.at[1]),
        pltpu.make_async_copy(b1_hbm, b1_v, small_sem.at[2]),
        pltpu.make_async_copy(g2_hbm, g2_v, small_sem.at[3]),
        pltpu.make_async_copy(b2_hbm, b2_v, small_sem.at[4]),
        pltpu.make_async_copy(inv_hbm, inv_v, small_sem.at[5]),
    ]
    for cp in smalls:
        cp.start()
    for g in range(ngrp):
        for t in range(3):
            qkv_copy(g, t).start(priority=1)
    for n in range(2):
        b_copy(n).start(priority=1)

    barrier = pltpu.get_barrier_semaphore()
    pl.semaphore_signal(barrier, inc=1, device_id={"seq": partner}, device_id_type=MESH)
    for i in range(1, nchip):
        pl.semaphore_signal(barrier, inc=1, device_id=dev(lax.rem(me + i, nchip)), device_id_type=MESH)

    def norms(which):
        xf = xall[which].astype(F32)
        mu = jnp.mean(xf, axis=-1, keepdims=True)
        xc = xf - mu
        var = jnp.mean(jnp.square(xc), axis=-1, keepdims=True)
        xn = xc * lax.rsqrt(var + EPS)
        a_v[which] = (xn * g1_v[...].reshape(1, d) + b1_v[...].reshape(1, d)).astype(BF16)
        m_v[which] = (xn * g2_v[...].reshape(1, d) + b2_v[...].reshape(1, d)).astype(BF16)

    for cp in smalls[:5]:
        cp.wait()
    norms(c)

    smalls[5].wait()
    pos = (me * r2 + lax.broadcasted_iota(jnp.int32, (r2, 128), 0)).astype(F32)
    ang = pos * inv_v[0:1, :]
    cos = jnp.cos(ang)
    sin = jnp.sin(ang)
    lane = lax.broadcasted_iota(jnp.int32, (r2, 128), 1)
    sin = jnp.where(lane < half, -sin, sin)
    cs[0] = jnp.concatenate([cos[:, :dh]] * GH, axis=1).reshape(2, r, cw)
    cs[1] = jnp.concatenate([sin[:, :dh]] * GH, axis=1).reshape(2, r, cw)

    lane_c = lax.rem(lax.broadcasted_iota(jnp.int32, (r, cw), 1), dh)

    def rope(t, which):
        tf = t.astype(F32)
        up = pltpu.roll(tf, cw - half, axis=1)
        dn = pltpu.roll(tf, half, axis=1)
        rot = jnp.where(lane_c < half, up, dn)
        return (tf * cs[0, which] + rot * cs[1, which]).astype(BF16)

    def q_send(src, chip, which):
        return pltpu.make_async_remote_copy(
            src_ref=sbuf.at[chip, which], dst_ref=rbuf.at[pl.ds(pl.multiple_of(src * r2 + which * r, r), r), :],
            send_sem=qs_sem.at[which, chip], recv_sem=qr_sem.at[which, src], device_id=dev(chip), device_id_type=MESH)

    def q_local(which):
        return pltpu.make_async_copy(
            sbuf.at[me, which], rbuf.at[pl.ds(pl.multiple_of(me * r2 + which * r, r), r), :], loc_sem.at[which])

    def q_part(g, which, t):
        part = jnp.dot(a_v[which], aw[3 * g + t], preferred_element_type=F32).astype(BF16)
        return rope(part, which) if t < 2 else part

    def q_pack(which, gg, parts):
        for j in range(GH):
            sl = slice(j * dh, (j + 1) * dh)
            sbuf[owner(gg, j), which] = jnp.concatenate(
                [parts[0][:, sl], parts[1][:, sl], parts[2][:, sl], jnp.zeros((r, 256 - 3 * dh), BF16)], axis=1)

    def q_group(g, gg):
        a = a_v[...].reshape(r2, d)
        parts = [jnp.dot(a, aw[3 * g + t], preferred_element_type=F32).astype(BF16) for t in range(3)]
        for which in range(2):
            pw = [p[which * r:(which + 1) * r] for p in parts]
            pw = [rope(pw[0], which), rope(pw[1], which), pw[2]]
            for j in range(GH):
                sl = slice(j * dh, (j + 1) * dh)
                sbuf[owner(gg, j), which] = jnp.concatenate(
                    [pw[0][:, sl], pw[1][:, sl], pw[2][:, sl], jnp.zeros((r, 256 - 3 * dh), BF16)], axis=1)

    def q_sends(gg, halves):
        def send(j, carry):
            chip = owner(gg, lax.rem(j + me // ngrp, GH))

            @pl.when(chip != me)
            def _():
                for which in halves:
                    q_send(me, chip, which).start()

            @pl.when(chip == me)
            def _():
                for which in halves:
                    q_local(which).start()
            return carry

        lax.fori_loop(0, GH, send, 0)

    parts = []
    qkv_copy(0, 0).wait()
    parts.append(q_part(0, c, 0))
    pl.semaphore_wait(barrier, nchip)
    xcopy = pltpu.make_async_remote_copy(
        src_ref=xall.at[c], dst_ref=xall.at[c], send_sem=xs_sem, recv_sem=xr_sem,
        device_id={"seq": partner}, device_id_type=MESH)
    xcopy.start()

    qkv_copy(0, 1).wait()
    parts.append(q_part(0, c, 1))
    qkv_copy(0, 2).wait()
    parts.append(q_part(0, c, 2))
    q_pack(c, group(0), parts)
    q_sends(group(0), [c])
    xcopy.wait()
    norms(1 - c)
    q_pack(1 - c, group(0), [q_part(0, 1 - c, t) for t in range(3)])
    for t in range(3):
        w1_copy(t).start(priority=1)
    q_sends(group(0), [1 - c])
    for g in range(1, ngrp):
        for t in range(3):
            qkv_copy(g, t).wait()
        q_group(g, group(g))
        for t in range(3):
            w1_copy(3 * g + t).start(priority=1)
        q_sends(group(g), [0, 1])

    def up(m):
        t_v[lax.rem(m, 2)] = jnp.dot(m_v[...].reshape(r2, d), aw[lax.rem(m, SLOTS)], preferred_element_type=F32)

    def act(m):
        h_v[:, pl.ds(pl.multiple_of(m * cw, 128), cw)] = _gelu(t_v[lax.rem(m, 2)]).astype(BF16)

    w1_copy(0).wait()
    up(0)
    w1_copy(SLOTS).start(priority=1)

    def mlp1(refill, m, carry):
        w1_copy(m).wait()
        act(m - 1)
        up(m)
        if refill:
            w1_copy(m + SLOTS).start(priority=1)
        return carry

    lax.fori_loop(1, nm - SLOTS, functools.partial(mlp1, True), 0)
    for n in range(2, nb2 + nbo):
        b_copy(n).start(priority=1)
    lax.fori_loop(nm - SLOTS, nm, functools.partial(mlp1, False), 0)
    act(nm - 1)

    nt = d // 2
    early = 2

    def down(k0, k1, first):
        def body(n, carry):
            cols = pl.ds(pl.multiple_of(n * nt, 128), nt)
            t = jnp.dot(h_v[:, k0:k1], bw[k0:k1, cols], preferred_element_type=F32).reshape(2, r, nt)
            yacc[:, :, cols] = t if first else yacc[:, :, cols] + t
            return carry

        lax.fori_loop(0, d // nt, body, 0)

    for n in range(early):
        b_copy(n).wait()
    down(0, early * cw, True)

    q_local(0).wait()
    q_local(1).wait()

    def q_wait(i, carry):
        chip = lax.rem(me + i, nchip)
        q_send(chip, chip, 0).wait()
        q_send(chip, chip, 1).wait()
        return carry

    lax.fori_loop(1, nchip, q_wait, 0)

    scale = dh ** -0.5 * math.log2(math.e)
    qper = KB // r2

    def o_send(src, chip):
        return pltpu.make_async_remote_copy(
            src_ref=obuf.at[chip], dst_ref=orecv.at[src],
            send_sem=os_sem.at[chip], recv_sem=or_sem.at[src], device_id=dev(chip), device_id_type=MESH)

    def o_local():
        return pltpu.make_async_copy(obuf.at[me], orecv.at[me], loc_sem.at[2])

    nq = nchip // qper
    og = r2 // 16

    def attend(i, carry):
        us = [lax.rem(me + i + n, qper) for n in range(nq)]
        blocks = [qper * n + us[n] for n in range(nq)]
        row0 = [pl.multiple_of(j * r2, r2) for j in blocks]
        lq = []
        for n in range(nq):
            q = rbuf[pl.ds(row0[n], r2), 0:128]
            lq.append(jnp.concatenate(
                [jnp.zeros((r2, dh), BF16), q[:, :dh], jnp.zeros((r2, 256 - 2 * dh), BF16)], axis=1))
        ahead = lax.broadcasted_iota(jnp.int32, (r2, KB), 1) - lax.broadcasted_iota(jnp.int32, (r2, KB), 0)
        sc = [[] for _ in range(nq)]
        for k in range(nq):
            t = lax.dot_general(jnp.concatenate(lq[k:], axis=0), rbuf[k * KB:(k + 1) * KB, :],
                                (((1,), (1,)), ((), ())), preferred_element_type=F32)
            for n in range(k, nq):
                tn = t[(n - k) * r2:(n - k + 1) * r2]
                sc[n].append(jnp.where(ahead <= us[n] * r2, tn, NEG) if n == k else tn)
        for n in range(nq):
            mx = functools.reduce(jnp.maximum, sc[n])
            mx = jnp.max(mx, axis=-1, keepdims=True)
            e = [jnp.exp2((t - mx) * scale) for t in sc[n]]
            inv_l = 1.0 / jnp.sum(functools.reduce(jnp.add, e), axis=-1, keepdims=True)
            p = jnp.concatenate([(t * inv_l).astype(BF16) for t in e], axis=1)
            o = jnp.dot(p, rbuf[0:(n + 1) * KB, 128:256], preferred_element_type=F32)
            v0 = 2 * dh - 128
            obuf[blocks[n]] = jnp.concatenate(
                [o[16 * g:16 * (g + 1), v0:v0 + dh] for g in range(og)], axis=1).astype(BF16)

        def send(n, carry):
            j = qper * n + lax.rem(me + i + n, qper)

            @pl.when(j != me)
            def _():
                o_send(me, j).start()

            @pl.when(j == me)
            def _():
                o_local().start()
            return carry

        lax.fori_loop(0, nq, send, 0)
        return carry

    lax.fori_loop(0, qper, attend, 0)

    for n in range(early, nb2):
        b_copy(n).wait()
    down(early * cw, fc, False)

    o_local().wait()

    def o_wait(i, carry):
        chip = lax.rem(me + i, nchip)
        o_send(chip, chip).wait()
        return carry

    lax.fori_loop(1, nchip, o_wait, 0)
    for g in range(og):
        ocat[16 * g:16 * (g + 1), :] = jnp.concatenate(
            [orecv[owner(j // GH, j % GH)][:, g * dh:(g + 1) * dh] for j in range(nchip)], axis=1)
    for n in range(nb2, nb2 + nbo):
        b_copy(n).wait()

    ny = 2
    yw = d // ny

    def y_send(n):
        cols = pl.ds(pl.multiple_of(n * yw, 128), yw)
        return pltpu.make_async_remote_copy(
            src_ref=yacc.at[1 - c, :, cols], dst_ref=yrecv.at[:, cols],
            send_sem=ys_sem.at[n], recv_sem=yr_sem.at[n], device_id={"seq": partner}, device_id_type=MESH)

    def proj(n, carry):
        cols = pl.ds(pl.multiple_of(n * yw, 128), yw)
        t = jnp.dot(ocat[...], bw[fc:fc + dc, cols], preferred_element_type=F32)
        yacc[:, :, cols] = yacc[:, :, cols] + t.reshape(2, r, yw)
        y_send(n).start()
        return carry

    lax.fori_loop(0, ny, proj, 0)

    def y_out(n):
        cols = pl.ds(pl.multiple_of(n * yw, 128), yw)
        return pltpu.make_async_copy(ybuf.at[:, cols], y_hbm.at[:, cols], out_sem.at[n])

    def finish(n, carry):
        cols = pl.ds(pl.multiple_of(n * yw, 128), yw)
        y_send(n).wait()
        ybuf[:, cols] = (xall[c, :, cols].astype(F32) + yacc[c, :, cols] + yrecv[:, cols]).astype(BF16)
        y_out(n).start()
        return carry

    lax.fori_loop(0, ny, finish, 0)
    for n in range(ny):
        y_out(n).wait()


def solution(mesh):
    nseq = mesh.shape["seq"]
    nchip = nseq // 2

    def local(x, g1, b1, g2, b2, wqkv, wo, w1, w2):
        r, d = x.shape
        nh, dh, _ = wo.shape
        f = w1.shape[1]
        if nh != nseq or nchip % GH or (KB % (2 * r)):
            raise ValueError("unsupported sizes")
        half = dh // 2
        inv = 10000.0 ** (-2.0 * np.arange(half) / dh)
        inv = np.concatenate([inv, inv, np.zeros(128 - dh)]).astype(np.float32)
        inv = jnp.asarray(np.tile(inv[None], (8, 1)))
        r2, cw, dc, fc = 2 * r, GH * dh, d // 2, f // 2
        nb = (fc + dc) // cw
        dma = pltpu.SemaphoreType.DMA
        flops = 2 * r2 * (d * 3 * dc + d * fc * 2 + dc * d)
        return pl.pallas_call(
            functools.partial(_kernel, (r, d, nh, dh, f, nchip)),
            out_shape=jax.ShapeDtypeStruct((r, d), BF16),
            in_specs=[pl.BlockSpec(memory_space=pl.ANY)] * 10,
            out_specs=pl.BlockSpec(memory_space=pl.ANY),
            scratch_shapes=[
                pltpu.VMEM((2, r, d), BF16),
                pltpu.VMEM((d,), F32),
                pltpu.VMEM((d,), F32),
                pltpu.VMEM((d,), F32),
                pltpu.VMEM((d,), F32),
                pltpu.VMEM((8, 128), F32),
                pltpu.VMEM((2, r, d), BF16),
                pltpu.VMEM((2, r, d), BF16),
                pltpu.VMEM((2, r2, cw), F32),
                pltpu.VMEM((r2, fc), BF16),
                pltpu.VMEM((SLOTS, d, cw), BF16),
                pltpu.VMEM((fc + dc, d), BF16),
                pltpu.VMEM((nchip, 2, r, 256), BF16),
                pltpu.VMEM((nchip * r2, 256), BF16),
                pltpu.VMEM((nchip, 16, r2 // 16 * dh), BF16),
                pltpu.VMEM((nchip, 16, r2 // 16 * dh), BF16),
                pltpu.VMEM((r2, dc), BF16),
                pltpu.VMEM((2, r, d), F32),
                pltpu.VMEM((r, d), F32),
                pltpu.VMEM((r, d), BF16),
                pltpu.VMEM((2, 2, r, cw), F32),
                dma((6,)), dma((SLOTS,)), dma((nb,)), dma, dma,
                dma((2, nchip)), dma((2, nchip)), dma((nchip,)), dma((nchip,)),
                dma((d // cw,)), dma((d // cw,)), dma((3,)), dma((d // cw,)),
            ],
            compiler_params=pltpu.CompilerParams(
                collective_id=0, has_side_effects=True, vmem_limit_bytes=67043328),
            cost_estimate=pl.CostEstimate(flops=flops, bytes_accessed=2 * (d * 3 * dc + d * f + dc * d), transcendentals=0),
            name="layer",
        )(x, g1, b1, g2, b2, inv,
          wqkv, wo.reshape(nh * dh, d), w1, w2)

    rows = P(("data", "seq"), None)
    rep = P()
    return jax.shard_map(local, mesh=mesh,
                         in_specs=(rows, rep, rep, rep, rep, rep, rep, rep, rep),
                         out_specs=rows, check_vma=False)
```

```python
import functools
import math

import jax
import jax.numpy as jnp
import numpy as np
from jax import lax
from jax.experimental import pallas as pl
from jax.experimental.pallas import tpu as pltpu
from jax.sharding import PartitionSpec as P

EPS = 1e-5
NEG = -1e30
F32 = jnp.float32
BF16 = jnp.bfloat16
MESH = pl.DeviceIdType.MESH
SLOTS = 6
GH = 8
KB = 512
FAR = (4, 5, 3, 6, 2, 7, 1)


def _gelu(x):
    return 0.5 * x * (1.0 + lax.erf(x * np.float32(math.sqrt(0.5))))


def _kernel(dims, x_hbm, g1_hbm, b1_hbm, g2_hbm, b2_hbm, inv_hbm, wqkv, wo, w1, w2, y_hbm,
            xall, g1_v, b1_v, g2_v, b2_v, inv_v, a_v, m_v, t_v, h_v, aw, bw, sbuf, rbuf, obuf, orecv, ocat, yacc, yrecv, ybuf, cs,
            small_sem, a_sem, b_sem, xs_sem, xr_sem, qs_sem, qr_sem, os_sem, or_sem, ys_sem, yr_sem, loc_sem, out_sem):
    r, d, nh, dh, f, nchip = dims
    half = dh // 2
    dc = d // 2
    fc = f // 2
    cw = GH * dh
    ngrp = nchip // GH
    nm = fc // cw
    r2 = 2 * r
    s = lax.axis_index("seq")
    c = lax.rem(s, 2)
    me = lax.div(s, 2)
    partner = s + 1 - 2 * c

    def dev(chip):
        return {"seq": 2 * chip + c}

    def owner(g, j):
        return ngrp * j + (j // 2 + g) % ngrp

    def group(g):
        return (me % ngrp + me // (2 * ngrp) + g + 1) % ngrp

    def qkv_copy(g, t):
        col = pl.multiple_of(t * d + c * dc + group(g) * cw, 128)
        n = 3 * g + t
        return pltpu.make_async_copy(wqkv.at[:, pl.ds(col, cw)], aw.at[n], a_sem.at[n])

    def w1_copy(m):
        col = pl.multiple_of(c * fc + m * cw, 128)
        n = lax.rem(m, SLOTS)
        return pltpu.make_async_copy(w1.at[:, pl.ds(col, cw)], aw.at[n], a_sem.at[n])

    nb2 = nm
    nbo = dc // cw

    def b_copy(n):
        if n < nb2:
            return pltpu.make_async_copy(w2.at[pl.ds(pl.multiple_of(c * fc + n * cw, 128), cw), :],
                                         bw.at[pl.ds(n * cw, cw), :], b_sem.at[n])
        k = n - nb2
        return pltpu.make_async_copy(wo.at[pl.ds(pl.multiple_of(c * dc + k * cw, 128), cw), :],
                                     bw.at[pl.ds(n * cw, cw), :], b_sem.at[n])

    smalls = [
        pltpu.make_async_copy(x_hbm, xall.at[c], small_sem.at[0]),
        pltpu.make_async_copy(g1_hbm, g1_v, small_sem.at[1]),
        pltpu.make_async_copy(b1_hbm, b1_v, small_sem.at[2]),
        pltpu.make_async_copy(g2_hbm, g2_v, small_sem.at[3]),
        pltpu.make_async_copy(b2_hbm, b2_v, small_sem.at[4]),
        pltpu.make_async_copy(inv_hbm, inv_v, small_sem.at[5]),
    ]
    for cp in smalls:
        cp.start()
    for g in range(ngrp):
        for t in range(3):
            qkv_copy(g, t).start(priority=1)
    for n in range(2):
        b_copy(n).start(priority=1)

    barrier = pltpu.get_barrier_semaphore()
    pl.semaphore_signal(barrier, inc=1, device_id={"seq": partner}, device_id_type=MESH)
    for i in range(1, nchip):
        pl.semaphore_signal(barrier, inc=1, device_id=dev(lax.rem(me + i, nchip)), device_id_type=MESH)

    def norms(which):
        xf = xall[which].astype(F32)
        mu = jnp.mean(xf, axis=-1, keepdims=True)
        xc = xf - mu
        var = jnp.mean(jnp.square(xc), axis=-1, keepdims=True)
        xn = xc * lax.rsqrt(var + EPS)
        a_v[which] = (xn * g1_v[...].reshape(1, d) + b1_v[...].reshape(1, d)).astype(BF16)
        m_v[which] = (xn * g2_v[...].reshape(1, d) + b2_v[...].reshape(1, d)).astype(BF16)

    for cp in smalls[:5]:
        cp.wait()
    norms(c)

    smalls[5].wait()
    pos = (me * r2 + lax.broadcasted_iota(jnp.int32, (r2, 128), 0)).astype(F32)
    ang = pos * inv_v[0:1, :]
    cos = jnp.cos(ang)
    sin = jnp.sin(ang)
    lane = lax.broadcasted_iota(jnp.int32, (r2, 128), 1)
    sin = jnp.where(lane < half, -sin, sin)
    cs[0] = jnp.concatenate([cos[:, :dh]] * GH, axis=1).reshape(2, r, cw)
    cs[1] = jnp.concatenate([sin[:, :dh]] * GH, axis=1).reshape(2, r, cw)

    lane_c = lax.rem(lax.broadcasted_iota(jnp.int32, (r, cw), 1), dh)

    def rope(t, which):
        tf = t.astype(F32)
        up = pltpu.roll(tf, cw - half, axis=1)
        dn = pltpu.roll(tf, half, axis=1)
        rot = jnp.where(lane_c < half, up, dn)
        return (tf * cs[0, which] + rot * cs[1, which]).astype(BF16)

    def q_send(src, chip, which):
        return pltpu.make_async_remote_copy(
            src_ref=sbuf.at[chip, which], dst_ref=rbuf.at[pl.ds(pl.multiple_of(src * r2 + which * r, r), r), :],
            send_sem=qs_sem.at[which, chip], recv_sem=qr_sem.at[which, src], device_id=dev(chip), device_id_type=MESH)

    def q_local(which):
        return pltpu.make_async_copy(
            sbuf.at[me, which], rbuf.at[pl.ds(pl.multiple_of(me * r2 + which * r, r), r), :], loc_sem.at[which])

    def q_part(g, which, t):
        part = jnp.dot(a_v[which], aw[3 * g + t], preferred_element_type=F32).astype(BF16)
        return rope(part, which) if t < 2 else part

    def q_pack(which, gg, parts):
        for j in range(GH):
            sl = slice(j * dh, (j + 1) * dh)
            sbuf[owner(gg, j), which] = jnp.concatenate(
                [parts[0][:, sl], parts[1][:, sl], parts[2][:, sl], jnp.zeros((r, 256 - 3 * dh), BF16)], axis=1)

    def q_group(g, gg):
        a = a_v[...].reshape(r2, d)
        parts = [jnp.dot(a, aw[3 * g + t], preferred_element_type=F32).astype(BF16) for t in range(3)]
        for which in range(2):
            pw = [p[which * r:(which + 1) * r] for p in parts]
            pw = [rope(pw[0], which), rope(pw[1], which), pw[2]]
            for j in range(GH):
                sl = slice(j * dh, (j + 1) * dh)
                sbuf[owner(gg, j), which] = jnp.concatenate(
                    [pw[0][:, sl], pw[1][:, sl], pw[2][:, sl], jnp.zeros((r, 256 - 3 * dh), BF16)], axis=1)

    def q_sends(gg, halves):
        for k in FAR:
            chip = owner(gg, (k + me // ngrp) % GH)
            for which in halves:
                q_send(me, chip, which).start()
        chip = owner(gg, me // ngrp)

        @pl.when(chip != me)
        def _():
            for which in halves:
                q_send(me, chip, which).start()

        @pl.when(chip == me)
        def _():
            for which in halves:
                q_local(which).start()

    parts = []
    qkv_copy(0, 0).wait()
    parts.append(q_part(0, c, 0))
    pl.semaphore_wait(barrier, nchip)
    xcopy = pltpu.make_async_remote_copy(
        src_ref=xall.at[c], dst_ref=xall.at[c], send_sem=xs_sem, recv_sem=xr_sem,
        device_id={"seq": partner}, device_id_type=MESH)
    xcopy.start()

    qkv_copy(0, 1).wait()
    parts.append(q_part(0, c, 1))
    qkv_copy(0, 2).wait()
    parts.append(q_part(0, c, 2))
    q_pack(c, group(0), parts)
    q_sends(group(0), [c])
    xcopy.wait()
    norms(1 - c)
    q_pack(1 - c, group(0), [q_part(0, 1 - c, t) for t in range(3)])
    for t in range(3):
        w1_copy(t).start(priority=1)
    q_sends(group(0), [1 - c])
    for g in range(1, ngrp):
        for t in range(3):
            qkv_copy(g, t).wait()
        q_group(g, group(g))
        for t in range(3):
            w1_copy(3 * g + t).start(priority=1)
        q_sends(group(g), [0, 1])

    def up(m):
        t_v[lax.rem(m, 2)] = jnp.dot(m_v[...].reshape(r2, d), aw[lax.rem(m, SLOTS)], preferred_element_type=F32)

    def act(m):
        h_v[:, pl.ds(pl.multiple_of(m * cw, 128), cw)] = _gelu(t_v[lax.rem(m, 2)]).astype(BF16)

    w1_copy(0).wait()
    up(0)
    w1_copy(SLOTS).start(priority=1)

    def mlp1(refill, m, carry):
        w1_copy(m).wait()
        act(m - 1)
        up(m)
        if refill:
            w1_copy(m + SLOTS).start(priority=1)
        else:
            @pl.when(m == nm - SLOTS)
            def _():
                for n in range(2, nb2 + nbo):
                    b_copy(n).start(priority=1)
        return carry

    lax.fori_loop(1, nm - SLOTS, functools.partial(mlp1, True), 0)
    lax.fori_loop(nm - SLOTS, nm, functools.partial(mlp1, False), 0)
    act(nm - 1)

    nt = d // 2
    early = 2

    def down(k0, k1, first):
        def body(n, carry):
            cols = pl.ds(pl.multiple_of(n * nt, 128), nt)
            t = jnp.dot(h_v[:, k0:k1], bw[k0:k1, cols], preferred_element_type=F32).reshape(2, r, nt)
            yacc[:, :, cols] = t if first else yacc[:, :, cols] + t
            return carry

        lax.fori_loop(0, d // nt, body, 0)

    for n in range(early):
        b_copy(n).wait()
    down(0, early * cw, True)

    q_local(0).wait()
    q_local(1).wait()

    def q_wait(i, carry):
        chip = lax.rem(me + i, nchip)
        q_send(chip, chip, 0).wait()
        q_send(chip, chip, 1).wait()
        return carry

    lax.fori_loop(1, nchip, q_wait, 0)

    scale = dh ** -0.5 * math.log2(math.e)
    qper = KB // r2

    def o_send(src, chip):
        return pltpu.make_async_remote_copy(
            src_ref=obuf.at[chip], dst_ref=orecv.at[src],
            send_sem=os_sem.at[chip], recv_sem=or_sem.at[src], device_id=dev(chip), device_id_type=MESH)

    def o_local():
        return pltpu.make_async_copy(obuf.at[me], orecv.at[me], loc_sem.at[2])

    nq = nchip // qper
    og = r2 // 16

    def attend(i, carry):
        u = (me + jnp.where(i == qper - 1, 0, jnp.where(i == qper - 2, qper - 1, qper - 2 - i))) % qper
        blocks = [qper * n + u for n in range(nq)]
        row0 = [pl.multiple_of(j * r2, r2) for j in blocks]
        lq = []
        for n in range(nq):
            q = rbuf[pl.ds(row0[n], r2), 0:128]
            lq.append(jnp.concatenate(
                [jnp.zeros((r2, dh), BF16), q[:, :dh], jnp.zeros((r2, 256 - 2 * dh), BF16)], axis=1))
        seen = (lax.broadcasted_iota(jnp.int32, (r2, KB), 1) - lax.broadcasted_iota(jnp.int32, (r2, KB), 0)) <= u * r2
        sc = [[] for _ in range(nq)]
        for k in range(nq):
            t = lax.dot_general(jnp.concatenate(lq[k:], axis=0), rbuf[k * KB:(k + 1) * KB, :],
                                (((1,), (1,)), ((), ())), preferred_element_type=F32)
            for n in range(k, nq):
                tn = t[(n - k) * r2:(n - k + 1) * r2]
                sc[n].append(jnp.where(seen, tn, NEG) if n == k else tn)
        for n in range(nq):
            mx = functools.reduce(jnp.maximum, sc[n])
            mx = jnp.max(mx, axis=-1, keepdims=True)
            e = [jnp.exp2((t - mx) * scale) for t in sc[n]]
            inv_l = 1.0 / jnp.sum(functools.reduce(jnp.add, e), axis=-1, keepdims=True)
            p = jnp.concatenate([(t * inv_l).astype(BF16) for t in e], axis=1)
            o = jnp.dot(p, rbuf[0:(n + 1) * KB, 128:256], preferred_element_type=F32)
            v0 = 2 * dh - 128
            obuf[blocks[n]] = jnp.concatenate(
                [o[16 * g:16 * (g + 1), v0:v0 + dh] for g in range(og)], axis=1).astype(BF16)

        for j in blocks:
            @pl.when(j != me)
            def _():
                o_send(me, j).start()

            @pl.when(j == me)
            def _():
                o_local().start()
        return carry

    lax.fori_loop(0, qper, attend, 0)

    for n in range(early, nb2):
        b_copy(n).wait()
    down(early * cw, fc, False)

    o_local().wait()

    def o_wait(i, carry):
        chip = lax.rem(me + i, nchip)
        o_send(chip, chip).wait()
        return carry

    lax.fori_loop(1, nchip, o_wait, 0)
    for g in range(og):
        ocat[16 * g:16 * (g + 1), :] = jnp.concatenate(
            [orecv[owner(j // GH, j % GH)][:, g * dh:(g + 1) * dh] for j in range(nchip)], axis=1)
    for n in range(nb2, nb2 + nbo):
        b_copy(n).wait()

    ny = 2
    yw = d // ny

    def y_send(n):
        cols = pl.ds(pl.multiple_of(n * yw, 128), yw)
        return pltpu.make_async_remote_copy(
            src_ref=yacc.at[1 - c, :, cols], dst_ref=yrecv.at[:, cols],
            send_sem=ys_sem.at[n], recv_sem=yr_sem.at[n], device_id={"seq": partner}, device_id_type=MESH)

    def proj(n, carry):
        cols = pl.ds(pl.multiple_of(n * yw, 128), yw)
        t = jnp.dot(ocat[...], bw[fc:fc + dc, cols], preferred_element_type=F32)
        yacc[:, :, cols] = yacc[:, :, cols] + t.reshape(2, r, yw)
        y_send(n).start()
        return carry

    lax.fori_loop(0, ny, proj, 0)

    def y_out(n):
        cols = pl.ds(pl.multiple_of(n * yw, 128), yw)
        return pltpu.make_async_copy(ybuf.at[:, cols], y_hbm.at[:, cols], out_sem.at[n])

    def finish(n, carry):
        cols = pl.ds(pl.multiple_of(n * yw, 128), yw)
        y_send(n).wait()
        ybuf[:, cols] = (xall[c, :, cols].astype(F32) + yacc[c, :, cols] + yrecv[:, cols]).astype(BF16)
        y_out(n).start()
        return carry

    lax.fori_loop(0, ny, finish, 0)
    for n in range(ny):
        y_out(n).wait()


def solution(mesh):
    nseq = mesh.shape["seq"]
    nchip = nseq // 2

    def local(x, g1, b1, g2, b2, wqkv, wo, w1, w2):
        r, d = x.shape
        nh, dh, _ = wo.shape
        f = w1.shape[1]
        if nh != nseq or nchip % GH or (KB % (2 * r)):
            raise ValueError("unsupported sizes")
        half = dh // 2
        inv = 10000.0 ** (-2.0 * np.arange(half) / dh)
        inv = np.concatenate([inv, inv, np.zeros(128 - dh)]).astype(np.float32)
        inv = jnp.asarray(np.tile(inv[None], (8, 1)))
        r2, cw, dc, fc = 2 * r, GH * dh, d // 2, f // 2
        nb = (fc + dc) // cw
        dma = pltpu.SemaphoreType.DMA
        flops = 2 * r2 * (d * 3 * dc + d * fc * 2 + dc * d)
        return pl.pallas_call(
            functools.partial(_kernel, (r, d, nh, dh, f, nchip)),
            out_shape=jax.ShapeDtypeStruct((r, d), BF16),
            in_specs=[pl.BlockSpec(memory_space=pl.ANY)] * 10,
            out_specs=pl.BlockSpec(memory_space=pl.ANY),
            scratch_shapes=[
                pltpu.VMEM((2, r, d), BF16),
                pltpu.VMEM((d,), F32),
                pltpu.VMEM((d,), F32),
                pltpu.VMEM((d,), F32),
                pltpu.VMEM((d,), F32),
                pltpu.VMEM((8, 128), F32),
                pltpu.VMEM((2, r, d), BF16),
                pltpu.VMEM((2, r, d), BF16),
                pltpu.VMEM((2, r2, cw), F32),
                pltpu.VMEM((r2, fc), BF16),
                pltpu.VMEM((SLOTS, d, cw), BF16),
                pltpu.VMEM((fc + dc, d), BF16),
                pltpu.VMEM((nchip, 2, r, 256), BF16),
                pltpu.VMEM((nchip * r2, 256), BF16),
                pltpu.VMEM((nchip, 16, r2 // 16 * dh), BF16),
                pltpu.VMEM((nchip, 16, r2 // 16 * dh), BF16),
                pltpu.VMEM((r2, dc), BF16),
                pltpu.VMEM((2, r, d), F32),
                pltpu.VMEM((r, d), F32),
                pltpu.VMEM((r, d), BF16),
                pltpu.VMEM((2, 2, r, cw), F32),
                dma((6,)), dma((SLOTS,)), dma((nb,)), dma, dma,
                dma((2, nchip)), dma((2, nchip)), dma((nchip,)), dma((nchip,)),
                dma((d // cw,)), dma((d // cw,)), dma((3,)), dma((d // cw,)),
            ],
            compiler_params=pltpu.CompilerParams(
                collective_id=0, has_side_effects=True, vmem_limit_bytes=67043328),
            cost_estimate=pl.CostEstimate(flops=flops, bytes_accessed=2 * (d * 3 * dc + d * f + dc * d), transcendentals=0),
            name="layer",
        )(x, g1, b1, g2, b2, inv,
          wqkv, wo.reshape(nh * dh, d), w1, w2)

    rows = P(("data", "seq"), None)
    rep = P()
    return jax.shard_map(local, mesh=mesh,
                         in_specs=(rows, rep, rep, rep, rep, rep, rep, rep, rep),
                         out_specs=rows, check_vma=False)
```

```python
import functools
import math

import jax
import jax.numpy as jnp
import numpy as np
from jax import lax
from jax.experimental import pallas as pl
from jax.experimental.pallas import tpu as pltpu
from jax.sharding import PartitionSpec as P

EPS = 1e-5
NEG = -1e30
F32 = jnp.float32
BF16 = jnp.bfloat16
MESH = pl.DeviceIdType.MESH
SLOTS = 5
GH = 8
KB = 512
PW = 512
OSLOT = 0
FAR = (4, 5, 3, 6, 2, 7, 1)


def _gelu(x):
    return 0.5 * x * (1.0 + lax.erf(x * np.float32(math.sqrt(0.5))))


def _kernel(dims, x_hbm, g1_hbm, b1_hbm, g2_hbm, b2_hbm, inv_hbm, wqkv, wo, w1, w2, y_ref,
            xall, g1_v, b1_v, g2_v, b2_v, inv_v, a_v, m_v, h_v, aw, bw, sbuf, rbuf, obuf, orecv, yacc, yrecv, cs,
            small_sem, a_sem, b_sem, xs_sem, xr_sem, qs_sem, qr_sem, os_sem, or_sem, ys_sem, yr_sem, loc_sem):
    r, d, nh, dh, f, nchip = dims
    half = dh // 2
    dc = d // 2
    fc = f // 2
    cw = GH * dh
    ngrp = nchip // GH
    nm = fc // cw
    r2 = 2 * r
    s = lax.axis_index("seq")
    c = lax.rem(s, 2)
    me = lax.div(s, 2)
    partner = s + 1 - 2 * c

    def dev(chip):
        return {"seq": 2 * chip + c}

    def owner(g, j):
        return ngrp * j + (j // 2 + g) % ngrp

    def group(g):
        return (me % ngrp + me // (2 * ngrp) + g + 1) % ngrp

    def q_block(n):
        return aw.at[n] if n < SLOTS else bw.at[fc - d:fc, 0:cw]

    def qkv_copy(g, t):
        col = pl.multiple_of(t * d + c * dc + group(g) * cw, 128)
        n = 3 * g + t
        return pltpu.make_async_copy(wqkv.at[:, pl.ds(col, cw)], q_block(n), a_sem.at[n])

    def w1_copy(m):
        col = pl.multiple_of(c * fc + m * cw, 128)
        n = m % SLOTS
        return pltpu.make_async_copy(w1.at[:, pl.ds(col, cw)], aw.at[n], a_sem.at[n])

    nb2 = nm
    nbo = d // PW

    def b_copy(n):
        return pltpu.make_async_copy(w2.at[pl.ds(pl.multiple_of(c * fc + n * cw, 128), cw), :],
                                     bw.at[pl.ds(n * cw, cw), :], b_sem.at[n])

    def o_block(n):
        return aw.at[OSLOT + n // 2, pl.ds(n % 2 * dc, dc), 0:PW]

    def wo_copy(n):
        return pltpu.make_async_copy(wo.at[pl.ds(pl.multiple_of(c * dc, 128), dc), pl.ds(n * PW, PW)],
                                     o_block(n), b_sem.at[nb2 + n])

    smalls = [
        pltpu.make_async_copy(x_hbm, xall.at[c], small_sem.at[0]),
        pltpu.make_async_copy(g1_hbm, g1_v, small_sem.at[1]),
        pltpu.make_async_copy(b1_hbm, b1_v, small_sem.at[2]),
        pltpu.make_async_copy(g2_hbm, g2_v, small_sem.at[3]),
        pltpu.make_async_copy(b2_hbm, b2_v, small_sem.at[4]),
        pltpu.make_async_copy(inv_hbm, inv_v, small_sem.at[5]),
    ]
    for cp in smalls:
        cp.start()
    for n in range(3 * ngrp):
        qkv_copy(n // 3, n % 3).start(priority=1)
    for n in range(2):
        b_copy(n).start(priority=1)

    barrier = pltpu.get_barrier_semaphore()
    pl.semaphore_signal(barrier, inc=1, device_id={"seq": partner}, device_id_type=MESH)
    for i in range(1, nchip):
        pl.semaphore_signal(barrier, inc=1, device_id=dev(lax.rem(me + i, nchip)), device_id_type=MESH)

    def norms(which):
        xf = xall[which].astype(F32)
        mu = jnp.mean(xf, axis=-1, keepdims=True)
        xc = xf - mu
        var = jnp.mean(jnp.square(xc), axis=-1, keepdims=True)
        xn = xc * lax.rsqrt(var + EPS)
        a_v[which] = (xn * g1_v[...].reshape(1, d) + b1_v[...].reshape(1, d)).astype(BF16)
        m_v[which] = (xn * g2_v[...].reshape(1, d) + b2_v[...].reshape(1, d)).astype(BF16)

    for cp in smalls[:5]:
        cp.wait()
    norms(c)

    smalls[5].wait()
    pos = (me * r2 + lax.broadcasted_iota(jnp.int32, (r2, 128), 0)).astype(F32)
    ang = pos * inv_v[0:1, :]
    cos = jnp.cos(ang)
    sin = jnp.sin(ang)
    lane = lax.broadcasted_iota(jnp.int32, (r2, 128), 1)
    sin = jnp.where(lane < half, -sin, sin)
    cs[0] = jnp.concatenate([cos[:, :dh]] * GH, axis=1).reshape(2, r, cw)
    cs[1] = jnp.concatenate([sin[:, :dh]] * GH, axis=1).reshape(2, r, cw)

    lane_c = lax.rem(lax.broadcasted_iota(jnp.int32, (r, cw), 1), dh)

    def rope(t, which):
        tf = t.astype(F32)
        up = pltpu.roll(tf, cw - half, axis=1)
        dn = pltpu.roll(tf, half, axis=1)
        rot = jnp.where(lane_c < half, up, dn)
        return (tf * cs[0, which] + rot * cs[1, which]).astype(BF16)

    def q_send(src, chip, which):
        return pltpu.make_async_remote_copy(
            src_ref=sbuf.at[chip, which], dst_ref=rbuf.at[pl.ds(pl.multiple_of(src * r2 + which * r, r), r), :],
            send_sem=qs_sem.at[which, chip], recv_sem=qr_sem.at[which, src], device_id=dev(chip), device_id_type=MESH)

    def q_local(which):
        return pltpu.make_async_copy(
            sbuf.at[me, which], rbuf.at[pl.ds(pl.multiple_of(me * r2 + which * r, r), r), :], loc_sem.at[which])

    def q_part(g, which, t):
        part = jnp.dot(a_v[which], q_block(3 * g + t)[...], preferred_element_type=F32).astype(BF16)
        return rope(part, which) if t < 2 else part

    def q_pack(which, gg, parts):
        for j in range(GH):
            sl = slice(j * dh, (j + 1) * dh)
            sbuf[owner(gg, j), which] = jnp.concatenate(
                [parts[0][:, sl], parts[1][:, sl], parts[2][:, sl], jnp.zeros((r, 256 - 3 * dh), BF16)], axis=1)

    def q_group(g, gg):
        a = a_v[...].reshape(r2, d)
        for t in range(3):
            qkv_copy(g, t).wait()
        parts = [jnp.dot(a, q_block(3 * g + t)[...], preferred_element_type=F32).astype(BF16) for t in range(3)]
        for which in range(2):
            pw = [p[which * r:(which + 1) * r] for p in parts]
            pw = [rope(pw[0], which), rope(pw[1], which), pw[2]]
            for j in range(GH):
                sl = slice(j * dh, (j + 1) * dh)
                sbuf[owner(gg, j), which] = jnp.concatenate(
                    [pw[0][:, sl], pw[1][:, sl], pw[2][:, sl], jnp.zeros((r, 256 - 3 * dh), BF16)], axis=1)

    def q_sends(gg, halves):
        for k in FAR:
            chip = owner(gg, (k + me // ngrp) % GH)
            for which in halves:
                q_send(me, chip, which).start()
        chip = owner(gg, me // ngrp)

        @pl.when(chip != me)
        def _():
            for which in halves:
                q_send(me, chip, which).start()

        @pl.when(chip == me)
        def _():
            for which in halves:
                q_local(which).start()

    parts = []
    qkv_copy(0, 0).wait()
    parts.append(q_part(0, c, 0))
    pl.semaphore_wait(barrier, nchip)
    xcopy = pltpu.make_async_remote_copy(
        src_ref=xall.at[c], dst_ref=xall.at[c], send_sem=xs_sem, recv_sem=xr_sem,
        device_id={"seq": partner}, device_id_type=MESH)
    xcopy.start()

    qkv_copy(0, 1).wait()
    parts.append(q_part(0, c, 1))
    qkv_copy(0, 2).wait()
    parts.append(q_part(0, c, 2))
    q_pack(c, group(0), parts)
    q_sends(group(0), [c])
    xcopy.wait()
    norms(1 - c)
    q_pack(1 - c, group(0), [q_part(0, 1 - c, t) for t in range(3)])
    for n in range(3):
        w1_copy(n).start(priority=1)
    q_sends(group(0), [1 - c])
    for g in range(1, ngrp):
        q_group(g, group(g))
        for n in range(3 * g, min(3 * g + 3, SLOTS)):
            w1_copy(n).start(priority=1)
        q_sends(group(g), [0, 1])

    def pre(m):
        return pl.ds(pl.multiple_of(m % 2 * cw, 128), cw)

    def up(m):
        t = jnp.dot(m_v[...].reshape(r2, d), aw[m % SLOTS], preferred_element_type=F32)
        yacc[:, :, pre(m)] = t.reshape(2, r, cw)

    def act(m):
        h_v[:, pl.ds(pl.multiple_of(m * cw, 128), cw)] = _gelu(yacc[:, :, pre(m)].reshape(r2, cw)).astype(BF16)

    w1_copy(0).wait()
    up(0)
    w1_copy(SLOTS).start(priority=1)

    def mlp1(refill, m, carry):
        w1_copy(m).wait()
        act(m - 1)
        up(m)
        if refill:
            w1_copy(m + SLOTS).start(priority=1)
        else:
            @pl.when(m == nm - SLOTS)
            def _():
                for n in range(2, nb2):
                    b_copy(n).start(priority=1)
        return carry

    lax.fori_loop(1, nm - SLOTS, functools.partial(mlp1, True), 0)
    lax.fori_loop(nm - SLOTS, nm, functools.partial(mlp1, False), 0)
    for n in range(nbo):
        wo_copy(n).start(priority=1)
    act(nm - 1)

    nt = d // 2
    early = 2

    def down(k0, k1, first):
        def body(n, carry):
            cols = pl.ds(pl.multiple_of(n * nt, 128), nt)
            t = jnp.dot(h_v[:, k0:k1], bw[k0:k1, cols], preferred_element_type=F32).reshape(2, r, nt)
            yacc[:, :, cols] = t if first else yacc[:, :, cols] + t
            return carry

        lax.fori_loop(0, d // nt, body, 0)

    for n in range(early):
        b_copy(n).wait()
    down(0, early * cw, True)

    q_local(0).wait()
    q_local(1).wait()

    def q_wait(i, carry):
        chip = lax.rem(me + i, nchip)
        q_send(chip, chip, 0).wait()
        q_send(chip, chip, 1).wait()
        return carry

    lax.fori_loop(1, nchip, q_wait, 0)

    scale = dh ** -0.5 * math.log2(math.e)
    qper = KB // r2

    def o_send(src, chip):
        return pltpu.make_async_remote_copy(
            src_ref=obuf.at[chip], dst_ref=orecv.at[src],
            send_sem=os_sem.at[chip], recv_sem=or_sem.at[src], device_id=dev(chip), device_id_type=MESH)

    def o_local():
        return pltpu.make_async_copy(obuf.at[me], orecv.at[me], loc_sem.at[2])

    nq = nchip // qper
    og = r2 // 16

    def attend(i, carry):
        u = (me + jnp.where(i == qper - 1, 0, jnp.where(i == qper - 2, qper - 1, qper - 2 - i))) % qper
        blocks = [qper * n + u for n in range(nq)]
        row0 = [pl.multiple_of(j * r2, r2) for j in blocks]
        lq = []
        for n in range(nq):
            q = rbuf[pl.ds(row0[n], r2), 0:128]
            lq.append(jnp.concatenate(
                [jnp.zeros((r2, dh), BF16), q[:, :dh], jnp.zeros((r2, 256 - 2 * dh), BF16)], axis=1))
        seen = (lax.broadcasted_iota(jnp.int32, (r2, KB), 1) - lax.broadcasted_iota(jnp.int32, (r2, KB), 0)) <= u * r2
        sc = [[] for _ in range(nq)]
        for k in range(nq):
            t = lax.dot_general(jnp.concatenate(lq[k:], axis=0), rbuf[k * KB:(k + 1) * KB, :],
                                (((1,), (1,)), ((), ())), preferred_element_type=F32)
            for n in range(k, nq):
                tn = t[(n - k) * r2:(n - k + 1) * r2]
                sc[n].append(jnp.where(seen, tn, NEG) if n == k else tn)
        for n in range(nq):
            mx = functools.reduce(jnp.maximum, sc[n])
            mx = jnp.max(mx, axis=-1, keepdims=True)
            e = [jnp.exp2((t - mx) * scale) for t in sc[n]]
            inv_l = 1.0 / jnp.sum(functools.reduce(jnp.add, e), axis=-1, keepdims=True)
            p = jnp.concatenate([(t * inv_l).astype(BF16) for t in e], axis=1)
            o = jnp.dot(p, rbuf[0:(n + 1) * KB, 128:256], preferred_element_type=F32)
            v0 = 2 * dh - 128
            obuf[blocks[n]] = jnp.concatenate(
                [o[16 * g:16 * (g + 1), v0:v0 + dh] for g in range(og)], axis=1).astype(BF16)

        for j in blocks:
            @pl.when(j != me)
            def _():
                o_send(me, j).start()

            @pl.when(j == me)
            def _():
                o_local().start()
        return carry

    lax.fori_loop(0, qper, attend, 0)

    for n in range(early, nb2):
        b_copy(n).wait()
    down(early * cw, fc, False)

    o_local().wait()

    def o_wait(i, carry):
        chip = lax.rem(me + i, nchip)
        o_send(chip, chip).wait()
        return carry

    lax.fori_loop(1, nchip, o_wait, 0)
    for g in range(og):
        a_v[16 * g // r, 16 * g % r:16 * g % r + 16, 0:dc] = jnp.concatenate(
            [orecv[owner(j // GH, j % GH)][:, g * dh:(g + 1) * dh] for j in range(nchip)], axis=1)
    for n in range(nbo):
        wo_copy(n).wait()

    pieces = [(k, min(k + 2, nbo)) for k in range(0, nbo, 2)]

    def y_send(n):
        cols = slice(pieces[n][0] * PW, pieces[n][1] * PW)
        return pltpu.make_async_remote_copy(
            src_ref=yacc.at[1 - c, :, cols], dst_ref=yrecv.at[:, cols],
            send_sem=ys_sem.at[n], recv_sem=yr_sem.at[n], device_id={"seq": partner}, device_id_type=MESH)

    o_all = a_v[:, :, 0:dc].reshape(r2, dc)
    for n, (k0, k1) in enumerate(pieces):
        for k in range(k0, k1):
            cols = slice(k * PW, (k + 1) * PW)
            t = jnp.dot(o_all, o_block(k)[...], preferred_element_type=F32)
            yacc[:, :, cols] = yacc[:, :, cols] + t.reshape(2, r, PW)
        y_send(n).start()

    for n, (k0, k1) in enumerate(pieces):
        cols = slice(k0 * PW, k1 * PW)
        y_send(n).wait()
        y_ref[:, cols] = (xall[c, :, cols].astype(F32) + yacc[c, :, cols] + yrecv[:, cols]).astype(BF16)


def solution(mesh):
    nseq = mesh.shape["seq"]
    nchip = nseq // 2

    def local(x, g1, b1, g2, b2, wqkv, wo, w1, w2):
        r, d = x.shape
        nh, dh, _ = wo.shape
        f = w1.shape[1]
        if nh != nseq or nchip % GH or (KB % (2 * r)):
            raise ValueError("unsupported sizes")
        half = dh // 2
        inv = 10000.0 ** (-2.0 * np.arange(half) / dh)
        inv = np.concatenate([inv, inv, np.zeros(128 - dh)]).astype(np.float32)
        inv = jnp.asarray(np.tile(inv[None], (8, 1)))
        r2, cw, dc, fc = 2 * r, GH * dh, d // 2, f // 2
        nb = fc // cw + d // PW
        dma = pltpu.SemaphoreType.DMA
        flops = 2 * r2 * (d * 3 * dc + d * fc * 2 + dc * d)
        return pl.pallas_call(
            functools.partial(_kernel, (r, d, nh, dh, f, nchip)),
            out_shape=jax.ShapeDtypeStruct((r, d), BF16),
            in_specs=[pl.BlockSpec(memory_space=pl.ANY)] * 10,
            out_specs=pl.BlockSpec(memory_space=pltpu.VMEM),
            scratch_shapes=[
                pltpu.VMEM((2, r, d), BF16),
                pltpu.VMEM((d,), F32),
                pltpu.VMEM((d,), F32),
                pltpu.VMEM((d,), F32),
                pltpu.VMEM((d,), F32),
                pltpu.VMEM((8, 128), F32),
                pltpu.VMEM((2, r, d), BF16),
                pltpu.VMEM((2, r, d), BF16),
                pltpu.VMEM((r2, fc), BF16),
                pltpu.VMEM((SLOTS, d, cw), BF16),
                pltpu.VMEM((fc, d), BF16),
                pltpu.VMEM((nchip, 2, r, 256), BF16),
                pltpu.VMEM((nchip * r2, 256), BF16),
                pltpu.VMEM((nchip, 16, r2 // 16 * dh), BF16),
                pltpu.VMEM((nchip, 16, r2 // 16 * dh), BF16),
                pltpu.VMEM((2, r, d), F32),
                pltpu.VMEM((r, d), F32),
                pltpu.VMEM((2, 2, r, cw), F32),
                dma((6,)), dma((6,)), dma((nb,)), dma, dma,
                dma((2, nchip)), dma((2, nchip)), dma((nchip,)), dma((nchip,)),
                dma((d // cw,)), dma((d // cw,)), dma((3,)),
            ],
            compiler_params=pltpu.CompilerParams(
                collective_id=0, has_side_effects=True, vmem_limit_bytes=55600000),
            cost_estimate=pl.CostEstimate(flops=flops, bytes_accessed=2 * (d * 3 * dc + d * f + dc * d), transcendentals=0),
            name="layer",
        )(*[pltpu.with_memory_space_constraint(v, pltpu.HBM)
            for v in (x, g1, b1, g2, b2, inv, wqkv, wo.reshape(nh * dh, d), w1, w2)])

    rows = P(("data", "seq"), None)
    rep = P()
    return jax.shard_map(local, mesh=mesh,
                         in_specs=(rows, rep, rep, rep, rep, rep, rep, rep, rep),
                         out_specs=rows, check_vma=False)
```

```python
import functools
import math

import jax
import jax.numpy as jnp
import numpy as np
from jax import lax
from jax.experimental import pallas as pl
from jax.experimental.pallas import tpu as pltpu
from jax.sharding import PartitionSpec as P

EPS = 1e-5
NEG = -1e30
F32 = jnp.float32
BF16 = jnp.bfloat16
MESH = pl.DeviceIdType.MESH
SLOTS = 5
GH = 8
KB = 512
PW = 512
OSLOT = 0
DX = (2, 1, 3, 0)
FAR = (4, 5, 3, 6, 2, 7, 1)


def _gelu(x):
    return 0.5 * x * (1.0 + lax.erf(x * np.float32(math.sqrt(0.5))))


def _kernel(dims, x_hbm, g1_hbm, b1_hbm, g2_hbm, b2_hbm, inv_hbm, wqkv, wo, w1, w2, y_ref,
            xall, g1_v, b1_v, g2_v, b2_v, inv_v, a_v, m_v, h_v, aw, bw, sbuf, rbuf, obuf, orecv, yacc, yrecv, cs,
            small_sem, a_sem, b_sem, xs_sem, xr_sem, qs_sem, qr_sem, os_sem, or_sem, ys_sem, yr_sem, loc_sem):
    r, d, nh, dh, f, nchip = dims
    half = dh // 2
    dc = d // 2
    fc = f // 2
    cw = GH * dh
    ngrp = nchip // GH
    nm = fc // cw
    r2 = 2 * r
    s = lax.axis_index("seq")
    c = lax.rem(s, 2)
    me = lax.div(s, 2)
    partner = s + 1 - 2 * c

    def dev(chip):
        return {"seq": 2 * chip + c}

    def owner(g, j):
        return ngrp * j + (j // 2 + g) % ngrp

    def group(g):
        return (me % ngrp + me // (2 * ngrp) + g + 1) % ngrp

    def q_block(n):
        return aw.at[n] if n < SLOTS else bw.at[fc - d:fc, 0:cw]

    def qkv_copy(g, t):
        col = pl.multiple_of(t * d + c * dc + group(g) * cw, 128)
        n = 3 * g + t
        return pltpu.make_async_copy(wqkv.at[:, pl.ds(col, cw)], q_block(n), a_sem.at[n])

    def w1_copy(m):
        col = pl.multiple_of(c * fc + m * cw, 128)
        n = m % SLOTS
        return pltpu.make_async_copy(w1.at[:, pl.ds(col, cw)], aw.at[n], a_sem.at[n])

    nb2 = nm
    nbo = d // PW

    def b_copy(n):
        return pltpu.make_async_copy(w2.at[pl.ds(pl.multiple_of(c * fc + n * cw, 128), cw), :],
                                     bw.at[pl.ds(n * cw, cw), :], b_sem.at[n])

    def o_block(n):
        return aw.at[OSLOT + n // 2, pl.ds(n % 2 * dc, dc), 0:PW]

    def wo_copy(n):
        return pltpu.make_async_copy(wo.at[pl.ds(pl.multiple_of(c * dc, 128), dc), pl.ds(n * PW, PW)],
                                     o_block(n), b_sem.at[nb2 + n])

    smalls = [
        pltpu.make_async_copy(x_hbm, xall.at[c], small_sem.at[0]),
        pltpu.make_async_copy(g1_hbm, g1_v, small_sem.at[1]),
        pltpu.make_async_copy(b1_hbm, b1_v, small_sem.at[2]),
        pltpu.make_async_copy(g2_hbm, g2_v, small_sem.at[3]),
        pltpu.make_async_copy(b2_hbm, b2_v, small_sem.at[4]),
        pltpu.make_async_copy(inv_hbm, inv_v, small_sem.at[5]),
    ]
    for cp in smalls:
        cp.start()
    for n in range(3 * ngrp):
        qkv_copy(n // 3, n % 3).start(priority=1)
    for n in range(2):
        b_copy(n).start(priority=1)

    barrier = pltpu.get_barrier_semaphore()
    pl.semaphore_signal(barrier, inc=1, device_id={"seq": partner}, device_id_type=MESH)
    for i in range(1, nchip):
        pl.semaphore_signal(barrier, inc=1, device_id=dev(lax.rem(me + i, nchip)), device_id_type=MESH)

    def norms(which):
        xf = xall[which].astype(F32)
        mu = jnp.mean(xf, axis=-1, keepdims=True)
        xc = xf - mu
        var = jnp.mean(jnp.square(xc), axis=-1, keepdims=True)
        xn = xc * lax.rsqrt(var + EPS)
        a_v[which] = (xn * g1_v[...].reshape(1, d) + b1_v[...].reshape(1, d)).astype(BF16)
        m_v[which] = (xn * g2_v[...].reshape(1, d) + b2_v[...].reshape(1, d)).astype(BF16)

    for cp in smalls[:5]:
        cp.wait()
    norms(c)

    smalls[5].wait()
    pos = (me * r2 + lax.broadcasted_iota(jnp.int32, (r2, 128), 0)).astype(F32)
    ang = pos * inv_v[0:1, :]
    cos = jnp.cos(ang)
    sin = jnp.sin(ang)
    lane = lax.broadcasted_iota(jnp.int32, (r2, 128), 1)
    sin = jnp.where(lane < half, -sin, sin)
    cs[0] = jnp.concatenate([cos[:, :dh]] * GH, axis=1).reshape(2, r, cw)
    cs[1] = jnp.concatenate([sin[:, :dh]] * GH, axis=1).reshape(2, r, cw)

    lane_c = lax.rem(lax.broadcasted_iota(jnp.int32, (r, cw), 1), dh)

    def rope(t, which):
        tf = t.astype(F32)
        up = pltpu.roll(tf, cw - half, axis=1)
        dn = pltpu.roll(tf, half, axis=1)
        rot = jnp.where(lane_c < half, up, dn)
        return (tf * cs[0, which] + rot * cs[1, which]).astype(BF16)

    def q_send(src, chip, which):
        return pltpu.make_async_remote_copy(
            src_ref=sbuf.at[chip, which], dst_ref=rbuf.at[pl.ds(pl.multiple_of(src * r2 + which * r, r), r), :],
            send_sem=qs_sem.at[which, chip], recv_sem=qr_sem.at[which, src], device_id=dev(chip), device_id_type=MESH)

    def q_local(which):
        return pltpu.make_async_copy(
            sbuf.at[me, which], rbuf.at[pl.ds(pl.multiple_of(me * r2 + which * r, r), r), :], loc_sem.at[which])

    def q_part(g, which, t):
        part = jnp.dot(a_v[which], q_block(3 * g + t)[...], preferred_element_type=F32).astype(BF16)
        return rope(part, which) if t < 2 else part

    def q_pack(which, gg, parts):
        for j in range(GH):
            sl = slice(j * dh, (j + 1) * dh)
            sbuf[owner(gg, j), which] = jnp.concatenate(
                [parts[0][:, sl], parts[1][:, sl], parts[2][:, sl], jnp.zeros((r, 256 - 3 * dh), BF16)], axis=1)

    def q_group(g, gg):
        a = a_v[...].reshape(r2, d)
        for t in range(3):
            qkv_copy(g, t).wait()
        parts = [jnp.dot(a, q_block(3 * g + t)[...], preferred_element_type=F32).astype(BF16) for t in range(3)]
        for which in range(2):
            pw = [p[which * r:(which + 1) * r] for p in parts]
            pw = [rope(pw[0], which), rope(pw[1], which), pw[2]]
            for j in range(GH):
                sl = slice(j * dh, (j + 1) * dh)
                sbuf[owner(gg, j), which] = jnp.concatenate(
                    [pw[0][:, sl], pw[1][:, sl], pw[2][:, sl], jnp.zeros((r, 256 - 3 * dh), BF16)], axis=1)

    def q_sends(gg, halves):
        for k in FAR:
            chip = owner(gg, (k + me // ngrp) % GH)
            for which in halves:
                q_send(me, chip, which).start()
        chip = owner(gg, me // ngrp)

        @pl.when(chip != me)
        def _():
            for which in halves:
                q_send(me, chip, which).start()

        @pl.when(chip == me)
        def _():
            for which in halves:
                q_local(which).start()

    parts = []
    qkv_copy(0, 0).wait()
    parts.append(q_part(0, c, 0))
    pl.semaphore_wait(barrier, nchip)
    xcopy = pltpu.make_async_remote_copy(
        src_ref=xall.at[c], dst_ref=xall.at[c], send_sem=xs_sem, recv_sem=xr_sem,
        device_id={"seq": partner}, device_id_type=MESH)
    xcopy.start()

    qkv_copy(0, 1).wait()
    parts.append(q_part(0, c, 1))
    qkv_copy(0, 2).wait()
    parts.append(q_part(0, c, 2))
    q_pack(c, group(0), parts)
    q_sends(group(0), [c])
    xcopy.wait()
    norms(1 - c)
    q_pack(1 - c, group(0), [q_part(0, 1 - c, t) for t in range(3)])
    for n in range(3):
        w1_copy(n).start(priority=1)
    q_sends(group(0), [1 - c])
    for g in range(1, ngrp):
        q_group(g, group(g))
        for n in range(3 * g, min(3 * g + 3, SLOTS)):
            w1_copy(n).start(priority=1)
        q_sends(group(g), [0, 1])

    def pre(m):
        return pl.ds(pl.multiple_of(m % 2 * cw, 128), cw)

    def up(m):
        t = jnp.dot(m_v[...].reshape(r2, d), aw[m % SLOTS], preferred_element_type=F32)
        yacc[:, :, pre(m)] = t.reshape(2, r, cw)

    def act(m):
        h_v[:, pl.ds(pl.multiple_of(m * cw, 128), cw)] = _gelu(yacc[:, :, pre(m)].reshape(r2, cw)).astype(BF16)

    w1_copy(0).wait()
    up(0)
    w1_copy(SLOTS).start(priority=1)

    def mlp1(refill, m, carry):
        w1_copy(m).wait()
        act(m - 1)
        up(m)
        if refill:
            w1_copy(m + SLOTS).start(priority=1)
        else:
            @pl.when(m == nm - SLOTS)
            def _():
                for n in range(2, nb2):
                    b_copy(n).start(priority=1)
        return carry

    lax.fori_loop(1, nm - SLOTS, functools.partial(mlp1, True), 0)
    lax.fori_loop(nm - SLOTS, nm, functools.partial(mlp1, False), 0)
    for n in range(nbo):
        wo_copy(n).start(priority=1)
    act(nm - 1)

    nt = d // 2
    early = 3

    def down(k0, k1, first):
        def body(n, carry):
            cols = pl.ds(pl.multiple_of(n * nt, 128), nt)
            t = jnp.dot(h_v[:, k0:k1], bw[k0:k1, cols], preferred_element_type=F32).reshape(2, r, nt)
            yacc[:, :, cols] = t if first else yacc[:, :, cols] + t
            return carry

        lax.fori_loop(0, d // nt, body, 0)

    for n in range(early):
        b_copy(n).wait()
    down(0, early * cw, True)

    q_local(0).wait()
    q_local(1).wait()

    def q_wait(i, carry):
        chip = lax.rem(me + i, nchip)
        q_send(chip, chip, 0).wait()
        q_send(chip, chip, 1).wait()
        return carry

    lax.fori_loop(1, nchip, q_wait, 0)

    scale = dh ** -0.5 * math.log2(math.e)
    qper = KB // r2

    def o_send(src, chip):
        return pltpu.make_async_remote_copy(
            src_ref=obuf.at[chip], dst_ref=orecv.at[src],
            send_sem=os_sem.at[chip], recv_sem=or_sem.at[src], device_id=dev(chip), device_id_type=MESH)

    def o_local():
        return pltpu.make_async_copy(obuf.at[me], orecv.at[me], loc_sem.at[2])

    nq = nchip // qper
    og = r2 // 16

    def attend(dx):
        u = (me + dx) % qper
        blocks = [qper * n + u for n in range(nq)]
        row0 = [pl.multiple_of(j * r2, r2) for j in blocks]
        lq = []
        for n in range(nq):
            q = rbuf[pl.ds(row0[n], r2), 0:128]
            lq.append(jnp.concatenate(
                [jnp.zeros((r2, dh), BF16), q[:, :dh], jnp.zeros((r2, 256 - 2 * dh), BF16)], axis=1))
        seen = (lax.broadcasted_iota(jnp.int32, (r2, KB), 1) - lax.broadcasted_iota(jnp.int32, (r2, KB), 0)) <= u * r2
        sc = [[] for _ in range(nq)]
        for k in range(nq):
            t = lax.dot_general(jnp.concatenate(lq[k:], axis=0), rbuf[k * KB:(k + 1) * KB, :],
                                (((1,), (1,)), ((), ())), preferred_element_type=F32)
            for n in range(k, nq):
                tn = t[(n - k) * r2:(n - k + 1) * r2]
                sc[n].append(jnp.where(seen, tn, NEG) if n == k else tn)
        for n in range(nq):
            mx = functools.reduce(jnp.maximum, sc[n])
            mx = jnp.max(mx, axis=-1, keepdims=True)
            e = [jnp.exp2((t - mx) * scale) for t in sc[n]]
            inv_l = 1.0 / jnp.sum(functools.reduce(jnp.add, e), axis=-1, keepdims=True)
            p = jnp.concatenate([(t * inv_l).astype(BF16) for t in e], axis=1)
            o = jnp.dot(p, rbuf[0:(n + 1) * KB, 128:256], preferred_element_type=F32)
            v0 = 2 * dh - 128
            obuf[blocks[n]] = jnp.concatenate(
                [o[16 * g:16 * (g + 1), v0:v0 + dh] for g in range(og)], axis=1).astype(BF16)

        return blocks

    def o_sends(dx, blocks):
        for j in blocks:
            if dx:
                o_send(me, j).start()
                continue

            @pl.when(j != me)
            def _():
                o_send(me, j).start()

            @pl.when(j == me)
            def _():
                o_local().start()

    first = [attend(dx) for dx in DX[:2]]
    for dx, blocks in zip(DX[:2], first):
        o_sends(dx, blocks)
    for dx in DX[2:]:
        o_sends(dx, attend(dx))

    for n in range(early, nb2):
        b_copy(n).wait()
    down(early * cw, fc, False)

    o_local().wait()

    def o_wait(i, carry):
        chip = lax.rem(me + i, nchip)
        o_send(chip, chip).wait()
        return carry

    lax.fori_loop(1, nchip, o_wait, 0)
    for g in range(og):
        a_v[16 * g // r, 16 * g % r:16 * g % r + 16, 0:dc] = jnp.concatenate(
            [orecv[owner(j // GH, j % GH)][:, g * dh:(g + 1) * dh] for j in range(nchip)], axis=1)
    for n in range(nbo):
        wo_copy(n).wait()

    pieces = [(k, min(k + 2, nbo)) for k in range(0, nbo, 2)]

    def y_send(n):
        cols = slice(pieces[n][0] * PW, pieces[n][1] * PW)
        return pltpu.make_async_remote_copy(
            src_ref=yacc.at[1 - c, :, cols], dst_ref=yrecv.at[:, cols],
            send_sem=ys_sem.at[n], recv_sem=yr_sem.at[n], device_id={"seq": partner}, device_id_type=MESH)

    o_all = a_v[:, :, 0:dc].reshape(r2, dc)
    for n, (k0, k1) in enumerate(pieces):
        for k in range(k0, k1):
            cols = slice(k * PW, (k + 1) * PW)
            t = jnp.dot(o_all, o_block(k)[...], preferred_element_type=F32)
            yacc[:, :, cols] = yacc[:, :, cols] + t.reshape(2, r, PW)
        y_send(n).start()

    for n, (k0, k1) in enumerate(pieces):
        cols = slice(k0 * PW, k1 * PW)
        y_send(n).wait()
        y_ref[:, cols] = (xall[c, :, cols].astype(F32) + yacc[c, :, cols] + yrecv[:, cols]).astype(BF16)


def solution(mesh):
    nseq = mesh.shape["seq"]
    nchip = nseq // 2

    def local(x, g1, b1, g2, b2, wqkv, wo, w1, w2):
        r, d = x.shape
        nh, dh, _ = wo.shape
        f = w1.shape[1]
        if nh != nseq or KB // (2 * r) != len(DX) or nchip % GH or (KB % (2 * r)):
            raise ValueError("unsupported sizes")
        half = dh // 2
        inv = 10000.0 ** (-2.0 * np.arange(half) / dh)
        inv = np.concatenate([inv, inv, np.zeros(128 - dh)]).astype(np.float32)
        inv = jnp.asarray(np.tile(inv[None], (8, 1)))
        r2, cw, dc, fc = 2 * r, GH * dh, d // 2, f // 2
        nb = fc // cw + d // PW
        dma = pltpu.SemaphoreType.DMA
        flops = 2 * r2 * (d * 3 * dc + d * fc * 2 + dc * d)
        return pl.pallas_call(
            functools.partial(_kernel, (r, d, nh, dh, f, nchip)),
            out_shape=jax.ShapeDtypeStruct((r, d), BF16),
            in_specs=[pl.BlockSpec(memory_space=pl.ANY)] * 10,
            out_specs=pl.BlockSpec(memory_space=pltpu.VMEM),
            scratch_shapes=[
                pltpu.VMEM((2, r, d), BF16),
                pltpu.VMEM((d,), F32),
                pltpu.VMEM((d,), F32),
                pltpu.VMEM((d,), F32),
                pltpu.VMEM((d,), F32),
                pltpu.VMEM((8, 128), F32),
                pltpu.VMEM((2, r, d), BF16),
                pltpu.VMEM((2, r, d), BF16),
                pltpu.VMEM((r2, fc), BF16),
                pltpu.VMEM((SLOTS, d, cw), BF16),
                pltpu.VMEM((fc, d), BF16),
                pltpu.VMEM((nchip, 2, r, 256), BF16),
                pltpu.VMEM((nchip * r2, 256), BF16),
                pltpu.VMEM((nchip, 16, r2 // 16 * dh), BF16),
                pltpu.VMEM((nchip, 16, r2 // 16 * dh), BF16),
                pltpu.VMEM((2, r, d), F32),
                pltpu.VMEM((r, d), F32),
                pltpu.VMEM((2, 2, r, cw), F32),
                dma((6,)), dma((6,)), dma((nb,)), dma, dma,
                dma((2, nchip)), dma((2, nchip)), dma((nchip,)), dma((nchip,)),
                dma((d // cw,)), dma((d // cw,)), dma((3,)),
            ],
            compiler_params=pltpu.CompilerParams(
                collective_id=0, has_side_effects=True, vmem_limit_bytes=55600000),
            cost_estimate=pl.CostEstimate(flops=flops, bytes_accessed=2 * (d * 3 * dc + d * f + dc * d), transcendentals=0),
            name="layer",
        )(*[pltpu.with_memory_space_constraint(v, pltpu.HBM)
            for v in (x, g1, b1, g2, b2, inv, wqkv, wo.reshape(nh * dh, d), w1, w2)])

    rows = P(("data", "seq"), None)
    rep = P()
    return jax.shard_map(local, mesh=mesh,
                         in_specs=(rows, rep, rep, rep, rep, rep, rep, rep, rep),
                         out_specs=rows, check_vma=False)
```

```python
import functools
import math

import jax
import jax.numpy as jnp
import numpy as np
from jax import lax
from jax.experimental import pallas as pl
from jax.experimental.pallas import tpu as pltpu
from jax.sharding import PartitionSpec as P

EPS = 1e-5
NEG = -1e30
F32 = jnp.float32
BF16 = jnp.bfloat16
MESH = pl.DeviceIdType.MESH
SLOTS = 5
GH = 8
KB = 512
PW = 512
OSLOT = 0
DX = (1, 3, 2, 0)
FAR = (4, 5, 3, 6, 2, 7, 1)


def _gelu(x):
    return 0.5 * x * (1.0 + lax.erf(x * np.float32(math.sqrt(0.5))))


def _kernel(dims, x_hbm, g1_hbm, b1_hbm, g2_hbm, b2_hbm, inv_hbm, wqkv, wo, w1, w2, y_ref,
            xall, g1_v, b1_v, g2_v, b2_v, inv_v, a_v, m_v, h_v, aw, bw, sbuf, rbuf, obuf, orecv, yacc, yrecv, cs,
            small_sem, a_sem, b_sem, xs_sem, xr_sem, qs_sem, qr_sem, os_sem, or_sem, ys_sem, yr_sem, loc_sem):
    r, d, nh, dh, f, nchip = dims
    half = dh // 2
    dc = d // 2
    fc = f // 2
    cw = GH * dh
    ngrp = nchip // GH
    nm = fc // cw
    r2 = 2 * r
    s = lax.axis_index("seq")
    c = lax.rem(s, 2)
    me = lax.div(s, 2)
    partner = s + 1 - 2 * c

    def dev(chip):
        return {"seq": 2 * chip + c}

    def owner(g, j):
        return ngrp * j + (j // 2 + g) % ngrp

    def group(g):
        return (me % ngrp + me // (2 * ngrp) + g + 1) % ngrp

    def q_block(n):
        return aw.at[n] if n < SLOTS else bw.at[fc - d:fc, 0:cw]

    def qkv_copy(g, t):
        col = pl.multiple_of(t * d + c * dc + group(g) * cw, 128)
        n = 3 * g + t
        return pltpu.make_async_copy(wqkv.at[:, pl.ds(col, cw)], q_block(n), a_sem.at[n])

    def w1_copy(m):
        col = pl.multiple_of(c * fc + m * cw, 128)
        n = m % SLOTS
        return pltpu.make_async_copy(w1.at[:, pl.ds(col, cw)], aw.at[n], a_sem.at[n])

    nb2 = nm
    nbo = d // PW

    def b_copy(n):
        return pltpu.make_async_copy(w2.at[pl.ds(pl.multiple_of(c * fc + n * cw, 128), cw), :],
                                     bw.at[pl.ds(n * cw, cw), :], b_sem.at[n])

    def o_block(n):
        return aw.at[OSLOT + n // 2, pl.ds(n % 2 * dc, dc), 0:PW]

    def wo_copy(n):
        return pltpu.make_async_copy(wo.at[pl.ds(pl.multiple_of(c * dc, 128), dc), pl.ds(n * PW, PW)],
                                     o_block(n), b_sem.at[nb2 + n])

    smalls = [
        pltpu.make_async_copy(x_hbm, xall.at[c], small_sem.at[0]),
        pltpu.make_async_copy(g1_hbm, g1_v, small_sem.at[1]),
        pltpu.make_async_copy(b1_hbm, b1_v, small_sem.at[2]),
        pltpu.make_async_copy(g2_hbm, g2_v, small_sem.at[3]),
        pltpu.make_async_copy(b2_hbm, b2_v, small_sem.at[4]),
        pltpu.make_async_copy(inv_hbm, inv_v, small_sem.at[5]),
    ]
    for cp in smalls:
        cp.start()
    for n in range(3 * ngrp):
        qkv_copy(n // 3, n % 3).start(priority=1)
    for n in range(2):
        b_copy(n).start(priority=1)

    barrier = pltpu.get_barrier_semaphore()
    pl.semaphore_signal(barrier, inc=1, device_id={"seq": partner}, device_id_type=MESH)
    for i in range(1, nchip):
        pl.semaphore_signal(barrier, inc=1, device_id=dev(lax.rem(me + i, nchip)), device_id_type=MESH)

    def norms(which):
        xf = xall[which].astype(F32)
        mu = jnp.mean(xf, axis=-1, keepdims=True)
        xc = xf - mu
        var = jnp.mean(jnp.square(xc), axis=-1, keepdims=True)
        xn = xc * lax.rsqrt(var + EPS)
        a_v[which] = (xn * g1_v[...].reshape(1, d) + b1_v[...].reshape(1, d)).astype(BF16)
        m_v[which] = (xn * g2_v[...].reshape(1, d) + b2_v[...].reshape(1, d)).astype(BF16)

    for cp in smalls[:5]:
        cp.wait()
    norms(c)

    smalls[5].wait()
    pos = (me * r2 + lax.broadcasted_iota(jnp.int32, (r2, 128), 0)).astype(F32)
    ang = pos * inv_v[0:1, :]
    cos = jnp.cos(ang)
    sin = jnp.sin(ang)
    lane = lax.broadcasted_iota(jnp.int32, (r2, 128), 1)
    sin = jnp.where(lane < half, -sin, sin)
    cs[0] = jnp.concatenate([cos[:, :dh]] * GH, axis=1).reshape(2, r, cw)
    cs[1] = jnp.concatenate([sin[:, :dh]] * GH, axis=1).reshape(2, r, cw)

    lane_c = lax.rem(lax.broadcasted_iota(jnp.int32, (r, cw), 1), dh)

    def rope(t, which):
        tf = t.astype(F32)
        up = pltpu.roll(tf, cw - half, axis=1)
        dn = pltpu.roll(tf, half, axis=1)
        rot = jnp.where(lane_c < half, up, dn)
        return (tf * cs[0, which] + rot * cs[1, which]).astype(BF16)

    def q_send(src, chip, which):
        return pltpu.make_async_remote_copy(
            src_ref=sbuf.at[chip, which], dst_ref=rbuf.at[pl.ds(pl.multiple_of(src * r2 + which * r, r), r), :],
            send_sem=qs_sem.at[which, chip], recv_sem=qr_sem.at[which, src], device_id=dev(chip), device_id_type=MESH)

    def q_local(which):
        return pltpu.make_async_copy(
            sbuf.at[me, which], rbuf.at[pl.ds(pl.multiple_of(me * r2 + which * r, r), r), :], loc_sem.at[which])

    def q_part(g, which, t):
        part = jnp.dot(a_v[which], q_block(3 * g + t)[...], preferred_element_type=F32).astype(BF16)
        return rope(part, which) if t < 2 else part

    def q_pack(which, gg, parts):
        for j in range(GH):
            sl = slice(j * dh, (j + 1) * dh)
            sbuf[owner(gg, j), which] = jnp.concatenate(
                [parts[0][:, sl], parts[1][:, sl], parts[2][:, sl], jnp.zeros((r, 256 - 3 * dh), BF16)], axis=1)

    def q_group(g, gg):
        a = a_v[...].reshape(r2, d)
        for t in range(3):
            qkv_copy(g, t).wait()
        parts = [jnp.dot(a, q_block(3 * g + t)[...], preferred_element_type=F32).astype(BF16) for t in range(3)]
        for which in range(2):
            pw = [p[which * r:(which + 1) * r] for p in parts]
            pw = [rope(pw[0], which), rope(pw[1], which), pw[2]]
            for j in range(GH):
                sl = slice(j * dh, (j + 1) * dh)
                sbuf[owner(gg, j), which] = jnp.concatenate(
                    [pw[0][:, sl], pw[1][:, sl], pw[2][:, sl], jnp.zeros((r, 256 - 3 * dh), BF16)], axis=1)

    def q_sends(gg, halves):
        for k in FAR:
            chip = owner(gg, (k + me // ngrp) % GH)
            for which in halves:
                q_send(me, chip, which).start()
        chip = owner(gg, me // ngrp)

        @pl.when(chip != me)
        def _():
            for which in halves:
                q_send(me, chip, which).start()

        @pl.when(chip == me)
        def _():
            for which in halves:
                q_local(which).start()

    parts = []
    qkv_copy(0, 0).wait()
    parts.append(q_part(0, c, 0))
    pl.semaphore_wait(barrier, nchip)
    xcopy = pltpu.make_async_remote_copy(
        src_ref=xall.at[c], dst_ref=xall.at[c], send_sem=xs_sem, recv_sem=xr_sem,
        device_id={"seq": partner}, device_id_type=MESH)
    xcopy.start()

    qkv_copy(0, 1).wait()
    parts.append(q_part(0, c, 1))
    qkv_copy(0, 2).wait()
    parts.append(q_part(0, c, 2))
    q_pack(c, group(0), parts)
    q_sends(group(0), [c])
    xcopy.wait()
    norms(1 - c)
    q_pack(1 - c, group(0), [q_part(0, 1 - c, t) for t in range(3)])
    for n in range(3):
        w1_copy(n).start(priority=1)
    q_sends(group(0), [1 - c])
    for g in range(1, ngrp):
        q_group(g, group(g))
        for n in range(3 * g, min(3 * g + 3, SLOTS)):
            w1_copy(n).start(priority=1)
        q_sends(group(g), [0, 1])

    def pre(m):
        return pl.ds(pl.multiple_of(m % 2 * cw, 128), cw)

    def up(m):
        t = jnp.dot(m_v[...].reshape(r2, d), aw[m % SLOTS], preferred_element_type=F32)
        yacc[:, :, pre(m)] = t.reshape(2, r, cw)

    def act(m):
        h_v[:, pl.ds(pl.multiple_of(m * cw, 128), cw)] = _gelu(yacc[:, :, pre(m)].reshape(r2, cw)).astype(BF16)

    w1_copy(0).wait()
    up(0)
    w1_copy(SLOTS).start(priority=1)

    def mlp1(refill, m, carry):
        w1_copy(m).wait()
        act(m - 1)
        up(m)
        if refill:
            w1_copy(m + SLOTS).start(priority=1)
        else:
            @pl.when(m == nm - SLOTS)
            def _():
                for n in range(2, nb2):
                    b_copy(n).start(priority=1)
        return carry

    lax.fori_loop(1, nm - SLOTS, functools.partial(mlp1, True), 0)
    lax.fori_loop(nm - SLOTS, nm, functools.partial(mlp1, False), 0)
    for n in range(nbo):
        wo_copy(n).start(priority=1)
    act(nm - 1)

    nt = d // 2
    early = 3

    def down(k0, k1, first):
        def body(n, carry):
            cols = pl.ds(pl.multiple_of(n * nt, 128), nt)
            t = jnp.dot(h_v[:, k0:k1], bw[k0:k1, cols], preferred_element_type=F32).reshape(2, r, nt)
            yacc[:, :, cols] = t if first else yacc[:, :, cols] + t
            return carry

        lax.fori_loop(0, d // nt, body, 0)

    for n in range(early):
        b_copy(n).wait()
    down(0, early * cw, True)

    q_local(0).wait()
    q_local(1).wait()

    def q_wait(i, carry):
        chip = lax.rem(me + i, nchip)
        q_send(chip, chip, 0).wait()
        q_send(chip, chip, 1).wait()
        return carry

    lax.fori_loop(1, nchip, q_wait, 0)

    scale = dh ** -0.5 * math.log2(math.e)
    qper = KB // r2

    def o_send(src, chip):
        return pltpu.make_async_remote_copy(
            src_ref=obuf.at[chip], dst_ref=orecv.at[src],
            send_sem=os_sem.at[chip], recv_sem=or_sem.at[src], device_id=dev(chip), device_id_type=MESH)

    def o_local():
        return pltpu.make_async_copy(obuf.at[me], orecv.at[me], loc_sem.at[2])

    nq = nchip // qper
    og = r2 // 16

    def attend(dx):
        u = (me + dx) % qper
        blocks = [qper * n + u for n in range(nq)]
        row0 = [pl.multiple_of(j * r2, r2) for j in blocks]
        lq = []
        for n in range(nq):
            q = rbuf[pl.ds(row0[n], r2), 0:128]
            lq.append(jnp.concatenate(
                [jnp.zeros((r2, dh), BF16), q[:, :dh], jnp.zeros((r2, 256 - 2 * dh), BF16)], axis=1))
        seen = (lax.broadcasted_iota(jnp.int32, (r2, KB), 1) - lax.broadcasted_iota(jnp.int32, (r2, KB), 0)) <= u * r2
        sc = [[] for _ in range(nq)]
        for k in range(nq):
            t = lax.dot_general(jnp.concatenate(lq[k:], axis=0), rbuf[k * KB:(k + 1) * KB, :],
                                (((1,), (1,)), ((), ())), preferred_element_type=F32)
            for n in range(k, nq):
                tn = t[(n - k) * r2:(n - k + 1) * r2]
                sc[n].append(jnp.where(seen, tn, NEG) if n == k else tn)
        for n in range(nq):
            mx = functools.reduce(jnp.maximum, sc[n])
            mx = jnp.max(mx, axis=-1, keepdims=True)
            e = [jnp.exp2((t - mx) * scale) for t in sc[n]]
            inv_l = 1.0 / jnp.sum(functools.reduce(jnp.add, e), axis=-1, keepdims=True)
            p = jnp.concatenate([(t * inv_l).astype(BF16) for t in e], axis=1)
            o = jnp.dot(p, rbuf[0:(n + 1) * KB, 128:256], preferred_element_type=F32)
            v0 = 2 * dh - 128
            obuf[blocks[n]] = jnp.concatenate(
                [o[16 * g:16 * (g + 1), v0:v0 + dh] for g in range(og)], axis=1).astype(BF16)

        return blocks

    def o_sends(dx, blocks):
        for j in blocks:
            if dx:
                o_send(me, j).start()
                continue

            @pl.when(j != me)
            def _():
                o_send(me, j).start()

            @pl.when(j == me)
            def _():
                o_local().start()

    first = [attend(dx) for dx in DX[:2]]
    for dx, blocks in zip(DX[:2], first):
        o_sends(dx, blocks)
    for dx in DX[2:]:
        o_sends(dx, attend(dx))

    for n in range(early, nb2):
        b_copy(n).wait()
    down(early * cw, fc, False)

    o_local().wait()

    def o_wait(i, carry):
        chip = lax.rem(me + i, nchip)
        o_send(chip, chip).wait()
        return carry

    lax.fori_loop(1, nchip, o_wait, 0)
    for g in range(og):
        a_v[16 * g // r, 16 * g % r:16 * g % r + 16, 0:dc] = jnp.concatenate(
            [orecv[owner(j // GH, j % GH)][:, g * dh:(g + 1) * dh] for j in range(nchip)], axis=1)
    for n in range(nbo):
        wo_copy(n).wait()

    pieces = [(k, min(k + 2, nbo)) for k in range(0, nbo, 2)]

    def y_send(n):
        cols = slice(pieces[n][0] * PW, pieces[n][1] * PW)
        return pltpu.make_async_remote_copy(
            src_ref=yacc.at[1 - c, :, cols], dst_ref=yrecv.at[:, cols],
            send_sem=ys_sem.at[n], recv_sem=yr_sem.at[n], device_id={"seq": partner}, device_id_type=MESH)

    o_all = a_v[:, :, 0:dc].reshape(r2, dc)
    for n, (k0, k1) in enumerate(pieces):
        for k in range(k0, k1):
            cols = slice(k * PW, (k + 1) * PW)
            t = jnp.dot(o_all, o_block(k)[...], preferred_element_type=F32)
            yacc[:, :, cols] = yacc[:, :, cols] + t.reshape(2, r, PW)
        y_send(n).start()

    for n, (k0, k1) in enumerate(pieces):
        cols = slice(k0 * PW, k1 * PW)
        y_send(n).wait()
        y_ref[:, cols] = (xall[c, :, cols].astype(F32) + yacc[c, :, cols] + yrecv[:, cols]).astype(BF16)


def solution(mesh):
    nseq = mesh.shape["seq"]
    nchip = nseq // 2

    def local(x, g1, b1, g2, b2, wqkv, wo, w1, w2):
        r, d = x.shape
        nh, dh, _ = wo.shape
        f = w1.shape[1]
        if nh != nseq or KB // (2 * r) != len(DX) or nchip % GH or (KB % (2 * r)):
            raise ValueError("unsupported sizes")
        half = dh // 2
        inv = 10000.0 ** (-2.0 * np.arange(half) / dh)
        inv = np.concatenate([inv, inv, np.zeros(128 - dh)]).astype(np.float32)
        inv = jnp.asarray(np.tile(inv[None], (8, 1)))
        r2, cw, dc, fc = 2 * r, GH * dh, d // 2, f // 2
        nb = fc // cw + d // PW
        dma = pltpu.SemaphoreType.DMA
        flops = 2 * r2 * (d * 3 * dc + d * fc * 2 + dc * d)
        return pl.pallas_call(
            functools.partial(_kernel, (r, d, nh, dh, f, nchip)),
            out_shape=jax.ShapeDtypeStruct((r, d), BF16),
            in_specs=[pl.BlockSpec(memory_space=pl.ANY)] * 10,
            out_specs=pl.BlockSpec(memory_space=pltpu.VMEM),
            scratch_shapes=[
                pltpu.VMEM((2, r, d), BF16),
                pltpu.VMEM((d,), F32),
                pltpu.VMEM((d,), F32),
                pltpu.VMEM((d,), F32),
                pltpu.VMEM((d,), F32),
                pltpu.VMEM((8, 128), F32),
                pltpu.VMEM((2, r, d), BF16),
                pltpu.VMEM((2, r, d), BF16),
                pltpu.VMEM((r2, fc), BF16),
                pltpu.VMEM((SLOTS, d, cw), BF16),
                pltpu.VMEM((fc, d), BF16),
                pltpu.VMEM((nchip, 2, r, 256), BF16),
                pltpu.VMEM((nchip * r2, 256), BF16),
                pltpu.VMEM((nchip, 16, r2 // 16 * dh), BF16),
                pltpu.VMEM((nchip, 16, r2 // 16 * dh), BF16),
                pltpu.VMEM((2, r, d), F32),
                pltpu.VMEM((r, d), F32),
                pltpu.VMEM((2, 2, r, cw), F32),
                dma((6,)), dma((6,)), dma((nb,)), dma, dma,
                dma((2, nchip)), dma((2, nchip)), dma((nchip,)), dma((nchip,)),
                dma((d // cw,)), dma((d // cw,)), dma((3,)),
            ],
            compiler_params=pltpu.CompilerParams(
                collective_id=0, has_side_effects=True, vmem_limit_bytes=55600000),
            cost_estimate=pl.CostEstimate(flops=flops, bytes_accessed=2 * (d * 3 * dc + d * f + dc * d), transcendentals=0),
            name="layer",
        )(*[pltpu.with_memory_space_constraint(v, pltpu.HBM)
            for v in (x, g1, b1, g2, b2, inv, wqkv, wo.reshape(nh * dh, d), w1, w2)])

    rows = P(("data", "seq"), None)
    rep = P()
    return jax.shard_map(local, mesh=mesh,
                         in_specs=(rows, rep, rep, rep, rep, rep, rep, rep, rep),
                         out_specs=rows, check_vma=False)
```
